32 devices in a mesh: dp: 1 (over z), tp: 4 (over y), cp: 8 (over x, core).
Axes of the slice: x: 4, y: 4, z: 1, core: 2. Of those that a mesh axis runs over, the one named last changes fastest.
The devices are a block of a 4x4x8 slice.
Arguments:
- hidden: bfloat16 [4096, 4096], P(('dp', 'cp'))
- tok_pos: int32 [4096], P(('dp', 'cp'))
- norm_gain: float32 [4096], replicated
- w_query: bfloat16 [4096, 4096], P(None, 'tp')
- w_key: bfloat16 [4096, 1024], P(None, 'tp')
- w_value: bfloat16 [4096, 1024], P(None, 'tp')
- w_out: bfloat16 [4096, 4096], P('tp')
Outputs:
- output 1: bfloat16 [4096, 4096], P(('dp', 'cp'))
- output 2: bfloat16 [4096, 8, 128], P(('dp', 'cp'), 'tp')
- output 3: bfloat16 [4096, 8, 128], P(('dp', 'cp'), 'tp')
All inputs are finite; a program needn't handle non-finite values.
Results may differ from the reference program's by a relative error of at most 0.00443208.
Values are sent between devices in bfloat16 or wider.
A program may use at most 768 MiB of HBM per device.

```python
import math
import jax
import jax.numpy as jnp
from jax import lax

D = 4096
HEADS = 32
KV_HEADS = 8
HEAD = 128
SEQ = 4096
RUN_LEN = 128
Q_BLOCK = 128
THETA = 1000000
EPS = 1e-5


def setup_inputs(seed: int = 0, part: int = 0) -> dict:
    shared = jax.random.split(jax.random.key(seed), 5)
    local = jax.random.split(jax.random.fold_in(jax.random.key(seed + 1), part), 4)
    run_order = jax.random.permutation(local[0], SEQ // RUN_LEN)
    tok_pos = (run_order[:, None] * RUN_LEN + jnp.arange(RUN_LEN)[None, :]).reshape(SEQ).astype(jnp.int32)
    waves = jax.random.normal(local[1], (4, D), jnp.float32)
    phases = jax.random.uniform(local[2], (4,), jnp.float32, 0.0, 2.0 * math.pi)
    cycles = jnp.array([0.5, 1.0, 1.5, 2.5], jnp.float32)
    angle = tok_pos.astype(jnp.float32)[:, None] * (cycles * (2.0 * math.pi / SEQ))[None, :] + phases[None, :]
    signal = jnp.dot(jnp.cos(angle), waves)
    noise = jax.random.normal(local[3], (SEQ, D), jnp.float32)
    hidden = (0.25 * signal + 0.2 * noise).astype(jnp.bfloat16)
    norm_gain = 1.0 + 0.3 * jax.random.normal(shared[0], (D,), jnp.float32)
    w_query = (jax.random.normal(shared[1], (D, HEADS * HEAD), jnp.float32) * D ** -0.5).astype(jnp.bfloat16)
    w_key = (jax.random.normal(shared[2], (D, KV_HEADS * HEAD), jnp.float32) * D ** -0.5).astype(jnp.bfloat16)
    w_value = (jax.random.normal(shared[3], (D, KV_HEADS * HEAD), jnp.float32) * D ** -0.5).astype(jnp.bfloat16)
    w_out = (jax.random.normal(shared[4], (HEADS * HEAD, D), jnp.float32) * (HEADS * HEAD) ** -0.5).astype(jnp.bfloat16)
    return {"hidden": hidden, "tok_pos": tok_pos, "norm_gain": norm_gain, "w_query": w_query, "w_key": w_key, "w_value": w_value, "w_out": w_out}


def rope_tables(tok_pos):
    inv_freq = 1.0 / (THETA ** (jnp.arange(0, HEAD, 2, dtype=jnp.float32) / HEAD))
    angles = tok_pos.astype(jnp.float32)[:, None] * inv_freq[None, :]
    return jnp.cos(angles)[:, None, :], jnp.sin(angles)[:, None, :]


def rotate_half(head_vecs, cos_tab, sin_tab):
    half_dim = head_vecs.shape[-1] // 2
    first_half = head_vecs[..., :half_dim].astype(jnp.float32)
    second_half = head_vecs[..., half_dim:].astype(jnp.float32)
    rotated = jnp.concatenate([first_half * cos_tab - second_half * sin_tab, second_half * cos_tab + first_half * sin_tab], axis=-1)
    return rotated.astype(jnp.bfloat16)


def reference(hidden, tok_pos, norm_gain, w_query, w_key, w_value, w_out):
    q_per_kv = HEADS // KV_HEADS
    n_blocks = SEQ // Q_BLOCK
    hid_f32 = hidden.astype(jnp.float32)
    normed = (hid_f32 * lax.rsqrt(jnp.mean(hid_f32 * hid_f32, axis=-1, keepdims=True) + EPS) * norm_gain).astype(jnp.bfloat16)
    queries = jnp.dot(normed, w_query, preferred_element_type=jnp.float32).astype(jnp.bfloat16).reshape(SEQ, HEADS, HEAD)
    keys_raw = jnp.dot(normed, w_key, preferred_element_type=jnp.float32).astype(jnp.bfloat16).reshape(SEQ, KV_HEADS, HEAD)
    values = jnp.dot(normed, w_value, preferred_element_type=jnp.float32).astype(jnp.bfloat16).reshape(SEQ, KV_HEADS, HEAD)
    cos_tab, sin_tab = rope_tables(tok_pos)
    q_rot = rotate_half(queries, cos_tab, sin_tab)
    k_rot = rotate_half(keys_raw, cos_tab, sin_tab)
    attn_scale = HEAD ** -0.5
    k_heads = jnp.transpose(k_rot, (1, 0, 2)).astype(jnp.float32)
    v_heads = jnp.transpose(values, (1, 0, 2)).astype(jnp.float32)
    q_blocks = jnp.transpose(q_rot.reshape(n_blocks, Q_BLOCK, KV_HEADS, q_per_kv, HEAD), (0, 2, 1, 3, 4))
    pos_blocks = tok_pos.reshape(n_blocks, Q_BLOCK)

    def one_block(block_in):
        q_blk, pos_blk = block_in
        allowed = tok_pos[None, :] <= pos_blk[:, None]

        def one_head(head_in):
            q_head, k_head, v_head = head_in
            scores = jnp.einsum("qgd,td->gqt", q_head.astype(jnp.float32), k_head) * attn_scale
            scores = jnp.where(allowed[None], scores, -jnp.inf)
            softmaxed = jax.nn.softmax(scores, axis=-1)
            return jnp.einsum("gqt,td->qgd", softmaxed, v_head)

        return lax.map(one_head, (q_blk, k_heads, v_heads))

    context = lax.map(one_block, (q_blocks, pos_blocks))
    attn_out = jnp.transpose(context, (0, 2, 1, 3, 4)).reshape(SEQ, HEADS * HEAD).astype(jnp.bfloat16)
    attn_proj = jnp.dot(attn_out, w_out, preferred_element_type=jnp.float32)
    return (hid_f32 + attn_proj).astype(jnp.bfloat16), k_rot, values
```

```python
import functools

import jax
import jax.numpy as jnp
from jax import lax
from jax.experimental import pallas as pl
from jax.experimental.pallas import tpu as pltpu
from jax.sharding import PartitionSpec as P

HEAD = 128
THETA = 1000000
EPS = 1e-5
NEG_BIG = -1e30
LOG2E = 1.4426950408889634
MESH = pl.DeviceIdType.MESH
VMEM_LIMIT = 64 * 2**20 - 64 * 2**10
POS_ROWS = 16
POS_BASE = 64


def vmem_spec():
    return pl.BlockSpec(memory_space=pltpu.VMEM)


def any_spec():
    return pl.BlockSpec(memory_space=pl.ANY)


def rope_tables(tok_pos):
    inv_freq = 1.0 / (THETA ** (jnp.arange(0, HEAD, 2, dtype=jnp.float32) / HEAD))
    angles = tok_pos.astype(jnp.float32)[:, None] * inv_freq[None, :]
    cos, sin = jnp.cos(angles), jnp.sin(angles)
    return jnp.concatenate([cos, cos], axis=-1), jnp.concatenate([-sin, sin], axis=-1)


def rope(head_f32, cos_full, sin_full):
    vals = head_f32.astype(jnp.bfloat16).astype(jnp.float32)
    return (vals * cos_full + pltpu.roll(vals, HEAD // 2, 1) * sin_full).astype(jnp.bfloat16)


def norm_kv_kernel(hid_ref, gain_ref, wk_ref, wv_ref, cos_ref, sin_ref, r_ref, k_ref, v_ref):
    x = hid_ref[...].astype(jnp.float32)
    scaled = x * lax.rsqrt(jnp.mean(x * x, axis=-1, keepdims=True) + EPS)
    normed = (scaled * gain_ref[...]).astype(jnp.bfloat16)
    r_ref[...] = normed
    k = jnp.dot(normed, wk_ref[...], preferred_element_type=jnp.float32)
    for h in range(k.shape[1] // HEAD):
        cols = slice(h * HEAD, (h + 1) * HEAD)
        k_ref[:, cols] = rope(k[:, cols], cos_ref[...], sin_ref[...])
    v_ref[...] = jnp.dot(normed, wv_ref[...], preferred_element_type=jnp.float32).astype(jnp.bfloat16)


def norm_kv(hidden, gain, wk, wv, cos_full, sin_full):
    rows, width = hidden.shape
    kv_cols = wk.shape[1]
    tile = rows // 2
    row_blk = lambda cols: pl.BlockSpec((tile, cols), lambda i: (i, 0))
    whole = lambda a: pl.BlockSpec(a.shape, lambda i: (0, 0))
    return pl.pallas_call(
        norm_kv_kernel,
        grid=(rows // tile,),
        in_specs=[row_blk(width), whole(gain), whole(wk), whole(wv), row_blk(HEAD), row_blk(HEAD)],
        out_specs=[row_blk(width), row_blk(kv_cols), row_blk(kv_cols)],
        out_shape=[
            jax.ShapeDtypeStruct((rows, width), jnp.bfloat16),
            jax.ShapeDtypeStruct((rows, kv_cols), jnp.bfloat16),
            jax.ShapeDtypeStruct((rows, kv_cols), jnp.bfloat16),
        ],
        compiler_params=pltpu.CompilerParams(dimension_semantics=("arbitrary",), vmem_limit_bytes=VMEM_LIMIT),
        name="norm_kv",
    )(hidden, gain, wk, wv, cos_full, sin_full)


def block_kernel(
    n_tp, n_x, kv_ref, r_ref, posq_ref, cos_ref, sin_ref, wq_ref, wo_ref, hid_ref, out_ref,
    kv, wq, wf, ct, q, mx, ls, acc, hs, ssem, rsem, lsem,
):
    rows, width = r_ref.shape
    heads = wq_ref.shape[1] // HEAD
    kv_heads = mx.shape[1]
    group = heads // kv_heads
    kv_cols = kv_heads * HEAD
    n_chunk, chunk = mx.shape[0], mx.shape[2] // group
    ctx_cols = heads * HEAD
    cols = width // n_tp
    half = rows // 2
    tp, cp = lax.axis_index("tp"), lax.axis_index("cp")
    x, core = cp // 2, cp % 2

    def at_x(dx, dc=0):
        return lax.rem(x + dx + n_x, n_x) * 2 + lax.rem(core + dc, 2)

    def at_y(dy):
        return lax.rem(tp + dy + n_tp, n_tp)

    x_right, x_left, partner = {"cp": at_x(1)}, {"cp": at_x(-1)}, {"cp": at_x(0, 1)}
    y_right, y_left, y_far = {"tp": at_y(1)}, {"tp": at_y(-1)}, {"tp": at_y(2)}

    def rc(src, dst, idx, dev):
        return pltpu.make_async_remote_copy(
            src_ref=src, dst_ref=dst, send_sem=ssem.at[idx], recv_sem=rsem.at[idx], device_id=dev, device_id_type=MESH
        )

    barrier = pltpu.get_barrier_semaphore()
    peers = (x_right, x_left, partner, y_right, y_left, y_far)
    for dev in peers:
        pl.semaphore_signal(barrier, inc=1, device_id=dev, device_id_type=MESH)
    pl.semaphore_wait(barrier, len(peers))

    top, low = pl.ds(0, half), pl.ds(half, half + POS_ROWS)
    kv_copies = [
        rc(kv_ref.at[top], kv.at[2, top], 0, x_right),
        rc(kv_ref.at[low], kv.at[3, low], 1, x_left),
        rc(kv_ref.at[low], kv.at[2, low], 2, x_right),
        rc(kv_ref.at[top], kv.at[3, top], 3, x_left),
        rc(kv_ref, kv.at[1], 4, partner),
        rc(kv.at[2, top], kv.at[6, top], 5, x_right),
        rc(kv.at[3, low], kv.at[6, low], 6, x_left),
        rc(kv.at[2], kv.at[4], 7, partner),
        rc(kv.at[3], kv.at[5], 8, partner),
        rc(kv.at[6], kv.at[7], 9, partner),
    ]
    for cpy in kv_copies[:5]:
        cpy.start()

    piece = wf.shape[1] // (2 * n_x)

    def w_rows(idx, part=None):
        if part is None:
            return pl.ds(pl.multiple_of(idx * piece, piece), piece)
        return pl.ds(pl.multiple_of(idx * piece + part * (piece // 2), piece // 2), piece // 2)

    def w_cols(t):
        return pl.ds(pl.multiple_of(t * cols, cols), cols)

    mine = w_rows(cp)
    w_swap = [
        rc(wo_ref.at[mine, w_cols(at_y(1))], wf.at[1, mine], 10, y_right),
        rc(wo_ref.at[mine, w_cols(at_y(-1))], wf.at[2, mine], 11, y_left),
        rc(wo_ref.at[mine, w_cols(at_y(2))], wf.at[3, mine], 12, y_far),
    ]
    for cpy in w_swap:
        cpy.start()

    n_q = 4
    q_cols = ctx_cols // n_q

    def wq_copy(c):
        sl = pl.ds(pl.multiple_of(c * q_cols, q_cols), q_cols)
        return pltpu.make_async_copy(wq_ref.at[:, sl], wq.at[c], lsem.at[c])

    for c in range(n_q):
        wq_copy(c).start()
    local = [
        pltpu.make_async_copy(kv_ref, kv.at[0], lsem.at[n_q]),
        pltpu.make_async_copy(wo_ref.at[:, w_cols(tp)], wf.at[0], lsem.at[n_q + 1]),
        pltpu.make_async_copy(hid_ref.at[:, w_cols(tp)], hs, lsem.at[n_q + 2]),
    ]
    for cpy in local:
        cpy.start()

    @pl.loop(0, n_q)
    def _(c):
        wq_copy(c).wait()
        qc = jnp.dot(r_ref[...], wq[c], preferred_element_type=jnp.float32)
        per = q_cols // HEAD
        for j in range(per):
            rot = rope(qc[:, j * HEAD : (j + 1) * HEAD], cos_ref[...], sin_ref[...])
            head = c * per + j
            kvh, g = head // group, lax.rem(head, group)
            for i in range(n_chunk):
                q[i, kvh, pl.ds(pl.multiple_of(g * chunk, chunk), chunk), :] = rot[i * chunk : (i + 1) * chunk]

    mx[...] = jnp.full_like(mx, NEG_BIG)
    ls[...] = jnp.zeros_like(ls)
    acc[...] = jnp.zeros_like(acc)
    scale = HEAD**-0.5 * LOG2E

    def attend(i, slot):
        pos_q = posq_ref[pl.ds(pl.multiple_of(i * chunk, chunk), chunk), :]
        hi = kv[slot, pl.ds(rows, 8), :].astype(jnp.float32)
        lo = kv[slot, pl.ds(rows + 8, 8), :].astype(jnp.float32)
        pos_k = (hi * POS_BASE + lo)[0:1, :]
        n_l = rows // HEAD
        bias = jnp.concatenate(
            [jnp.where(pos_k[:, t * HEAD : (t + 1) * HEAD] <= pos_q, 0.0, NEG_BIG) for t in range(n_l)], axis=1
        )
        for kvh in range(kv_heads):
            k_blk = kv[slot, pl.ds(0, rows), kvh * HEAD : (kvh + 1) * HEAD]
            v_blk = kv[slot, pl.ds(0, rows), kv_cols + kvh * HEAD : kv_cols + (kvh + 1) * HEAD]
            s = lax.dot_general(q[i, kvh], k_blk, (((1,), (1,)), ((), ())), preferred_element_type=jnp.float32)
            s = (s.reshape(group, chunk, rows) * scale + bias[None]).reshape(group * chunk, rows)
            m_old = mx[i, kvh]
            m_new = jnp.maximum(m_old, jnp.max(s, axis=1, keepdims=True))
            alpha = jnp.exp2(m_old - m_new)
            p = jnp.exp2(s - jnp.concatenate([m_new] * n_l, axis=1))
            part = p[:, :HEAD]
            for t in range(1, n_l):
                part = part + p[:, t * HEAD : (t + 1) * HEAD]
            mx[i, kvh] = m_new
            ls[i, kvh] = ls[i, kvh] * alpha + part
            acc[i, kvh] = acc[i, kvh] * alpha + jnp.dot(
                p.astype(jnp.bfloat16), v_blk, preferred_element_type=jnp.float32
            )

    def attend_pair(first):
        @pl.loop(0, 2 * n_chunk)
        def _(t):
            attend(t // 2, first + lax.rem(t, 2))

    for cpy in local:
        cpy.wait()
    kv_copies[0].wait_recv()
    kv_copies[5].start()
    kv_copies[1].wait_recv()
    kv_copies[6].start()
    kv_copies[4].wait_recv()
    attend_pair(0)

    for cpy in w_swap:
        cpy.wait_recv()

    def w_piece(idx, part=None):
        return wf.at[pl.ds(1, n_tp - 1), w_rows(idx, part)]

    own, right, left, far = cp, at_x(-1), at_x(1), at_x(2)

    def w_copy(src_idx, idx, dev, part=None):
        return rc(w_piece(src_idx, part), w_piece(src_idx, part), idx, dev)

    kv_copies[2].wait_recv()
    kv_copies[7].start()
    kv_copies[3].wait_recv()
    kv_copies[8].start()
    for idx, dev in ((13, x_right), (14, x_left), (15, partner)):
        w_copy(own, idx, dev).start()
    attend_pair(2)
    kv_copies[5].wait_recv()
    kv_copies[6].wait_recv()
    kv_copies[9].start()
    kv_copies[7].wait_recv()
    kv_copies[8].wait_recv()
    attend_pair(4)
    kv_copies[9].wait_recv()

    base = 24
    hc = chunk // 2

    def rows_of(i, part=None):
        if part is None:
            return pl.ds(pl.multiple_of(i * chunk, chunk), chunk)
        return pl.ds(pl.multiple_of(i * chunk + part * hc, hc), hc)

    def ctx_copies(i):
        sl = rows_of(i)
        first, second = rows_of(i, 0), rows_of(i, 1)
        b = base + 4 * i
        return (
            rc(ct.at[0, sl], ct.at[1, sl], b, y_right),
            rc(ct.at[0, sl], ct.at[2, sl], b + 1, y_left),
            rc(ct.at[1, first], ct.at[3, first], b + 2, y_right),
            rc(ct.at[2, second], ct.at[3, second], b + 3, y_left),
        )

    @pl.loop(0, n_chunk)
    def _(i):
        attend(i, 6)
        attend(i, 7)
        for kvh in range(kv_heads):
            total = jnp.sum(ls[i, kvh], axis=1, keepdims=True)
            ctx = (acc[i, kvh] / total).astype(jnp.bfloat16)
            for g in range(group):
                h = kvh * group + g
                ct[0, rows_of(i), h * HEAD : (h + 1) * HEAD] = ctx[g * chunk : (g + 1) * chunk]
        to_right, to_left, _, _ = ctx_copies(i)
        to_right.start()
        to_left.start()

    def ctx_forward(i):
        to_right, to_left, fwd_right, fwd_left = ctx_copies(i)
        to_right.wait_recv()
        fwd_right.start()
        to_left.wait_recv()
        fwd_left.start()

    ctx_forward(0)
    w_copy(right, 13, x_right).wait_recv()
    w_copy(right, 16, x_right, 0).start()
    w_copy(right, 18, partner).start()
    w_copy(left, 14, x_left).wait_recv()
    w_copy(left, 17, x_left, 1).start()
    w_copy(left, 19, partner).start()
    ctx_forward(1)
    ctx_forward(2)
    w_copy(far, 16, x_right, 0).wait_recv()
    w_copy(far, 17, x_left, 1).wait_recv()
    w_copy(far, 20, partner).start()
    ctx_forward(3)
    for idx, src in ((15, own), (18, right), (19, left), (20, far)):
        w_copy(src, idx, partner).wait_recv()

    out_base = base + 4 * n_chunk

    def out_copies(i):
        sl, first, second = rows_of(i), rows_of(i, 0), rows_of(i, 1)
        b = out_base + 4 * i
        mine_c, right_c, left_c = w_cols(tp), w_cols(at_y(-1)), w_cols(at_y(1))
        return (
            rc(out_ref.at[sl, mine_c], out_ref.at[sl, mine_c], b, y_right),
            rc(out_ref.at[sl, mine_c], out_ref.at[sl, mine_c], b + 1, y_left),
            rc(out_ref.at[first, right_c], out_ref.at[first, right_c], b + 2, y_right),
            rc(out_ref.at[second, left_c], out_ref.at[second, left_c], b + 3, y_left),
        )

    @pl.loop(0, n_chunk)
    def _(i):
        _, _, fwd_right, fwd_left = ctx_copies(i)
        fwd_right.wait_recv()
        fwd_left.wait_recv()
        sl = rows_of(i)
        y = hs[sl, :].astype(jnp.float32)
        proj = jnp.dot(ct[0, sl, :], wf[0], preferred_element_type=jnp.float32)
        for j in range(1, n_tp):
            proj = proj + jnp.dot(ct[j, sl, :], wf[j], preferred_element_type=jnp.float32)
        out_ref[sl, w_cols(tp)] = (y + proj).astype(jnp.bfloat16)
        to_right, to_left, _, _ = out_copies(i)
        to_right.start()
        to_left.start()

    @pl.loop(0, n_chunk)
    def _(i):
        to_right, to_left, fwd_right, fwd_left = out_copies(i)
        to_right.wait_recv()
        fwd_right.start()
        to_left.wait_recv()
        fwd_left.start()

    for cpy in kv_copies + w_swap:
        cpy.wait_send()
    for src, idx, dev, part in (
        (own, 13, x_right, None), (own, 14, x_left, None), (own, 15, partner, None), (right, 16, x_right, 0),
        (left, 17, x_left, 1), (right, 18, partner, None), (left, 19, partner, None), (far, 20, partner, None),
    ):
        w_copy(src, idx, dev, part).wait_send()

    @pl.loop(0, n_chunk)
    def _(i):
        for cpy in ctx_copies(i):
            cpy.wait_send()
        for cpy in out_copies(i):
            cpy.wait_send()
        _, _, fwd_right, fwd_left = out_copies(i)
        fwd_right.wait_recv()
        fwd_left.wait_recv()


def attention_block(mesh, kv_blk, normed, pos_q, cos_full, sin_full, w_query, w_out, hidden):
    n_tp, n_x = mesh.shape["tp"], mesh.shape["cp"] // 2
    rows, width = hidden.shape
    heads = w_query.shape[1] // HEAD
    kv_heads = kv_blk.shape[1] // (2 * HEAD)
    n_chunk = 4
    chunk = rows // n_chunk
    grp = heads // kv_heads * chunk
    bf16, f32 = jnp.bfloat16, jnp.float32
    n_sem = 24 + 8 * n_chunk
    return pl.pallas_call(
        functools.partial(block_kernel, n_tp, n_x),
        out_shape=jax.ShapeDtypeStruct((rows, width), bf16),
        in_specs=[vmem_spec()] * 5 + [any_spec()] * 3,
        out_specs=vmem_spec(),
        scratch_shapes=[
            pltpu.VMEM((2 * n_x, *kv_blk.shape), bf16),
            pltpu.VMEM((4, width, w_query.shape[1] // 4), bf16),
            pltpu.VMEM((n_tp, w_out.shape[0], width // n_tp), bf16),
            pltpu.VMEM((n_tp, rows, heads * HEAD), bf16),
            pltpu.VMEM((n_chunk, kv_heads, grp, HEAD), bf16),
            pltpu.VMEM((n_chunk, kv_heads, grp, HEAD), f32),
            pltpu.VMEM((n_chunk, kv_heads, grp, HEAD), f32),
            pltpu.VMEM((n_chunk, kv_heads, grp, HEAD), f32),
            pltpu.VMEM((rows, width // n_tp), bf16),
            pltpu.SemaphoreType.DMA((n_sem,)),
            pltpu.SemaphoreType.DMA((n_sem,)),
            pltpu.SemaphoreType.DMA((8,)),
        ],
        compiler_params=pltpu.CompilerParams(collective_id=0, has_side_effects=True, vmem_limit_bytes=VMEM_LIMIT),
        name="attention_block",
    )(kv_blk, normed, pos_q, cos_full, sin_full, w_query, w_out, hidden)


def solution(mesh):
    def local_block(hidden, tok_pos, norm_gain, w_query, w_key, w_value, w_out):
        rows = hidden.shape[0]
        kv_loc = w_key.shape[1] // HEAD
        cos_full, sin_full = rope_tables(tok_pos)
        normed, k_rot, values = norm_kv(hidden, norm_gain[None, :], w_key, w_value, cos_full, sin_full)
        pos_cols = jnp.stack([tok_pos // POS_BASE, tok_pos % POS_BASE]).astype(jnp.bfloat16)
        pos_rows = jnp.repeat(pos_cols, POS_ROWS // 2, axis=0)
        kv_blk = jnp.concatenate([jnp.concatenate([k_rot, values], axis=1), pos_rows], axis=0)
        pos_q = jnp.broadcast_to(tok_pos.astype(jnp.float32)[:, None], (rows, HEAD))
        hidden_out = attention_block(mesh, kv_blk, normed, pos_q, cos_full, sin_full, w_query, w_out, hidden)
        return hidden_out, k_rot.reshape(rows, kv_loc, HEAD), values.reshape(rows, kv_loc, HEAD)

    row_spec = P(("dp", "cp"), None)
    cache_spec = P(("dp", "cp"), "tp", None)
    return jax.shard_map(
        local_block,
        mesh=mesh,
        in_specs=(row_spec, P(("dp", "cp")), P(None), P(None, "tp"), P(None, "tp"), P(None, "tp"), P("tp", None)),
        out_specs=(row_spec, cache_spec, cache_spec),
        check_vma=False,
    )
```

```python
import functools

import jax
import jax.numpy as jnp
from jax import lax
from jax.experimental import pallas as pl
from jax.experimental.pallas import tpu as pltpu
from jax.sharding import PartitionSpec as P

HEAD = 128
THETA = 1000000
EPS = 1e-5
NEG_BIG = -1e30
LOG2E = 1.4426950408889634
MESH = pl.DeviceIdType.MESH
VMEM_LIMIT = 64 * 2**20 - 64 * 2**10
POS_ROWS = 16
POS_BASE = 64


def vmem_spec():
    return pl.BlockSpec(memory_space=pltpu.VMEM)


def any_spec():
    return pl.BlockSpec(memory_space=pl.ANY)


def inv_freq_row():
    freq = 1.0 / (THETA ** (jnp.arange(0, HEAD, 2, dtype=jnp.float32) / HEAD))
    return jnp.concatenate([freq, freq])[None, :]


def rope(head_f32, cos_full, sin_full):
    vals = head_f32.astype(jnp.bfloat16).astype(jnp.float32)
    return (vals * cos_full + pltpu.roll(vals, HEAD // 2, 1) * sin_full).astype(jnp.bfloat16)


def position_columns(pos_row):
    tiles = []
    for t in range(pos_row.shape[1] // HEAD):
        tile = jnp.broadcast_to(pos_row[:, t * HEAD : (t + 1) * HEAD], (HEAD, HEAD))
        tiles.append(jnp.transpose(tile))
    return jnp.concatenate(tiles, axis=0)


def norm_kv_kernel(
    pos_ref, freq_ref, gain_ref, hid_ref, wk_ref, wv_ref, r_out, kv_ref, cos_ref, sin_ref, kc_ref, vc_ref,
    hid, wk, wv, r, lsem,
):
    rows = hid.shape[0]
    kv_cols = wk.shape[1]
    n_part = 2
    part = rows // n_part

    def hid_copy(i):
        sl = slice(i * part, (i + 1) * part)
        return pltpu.make_async_copy(hid_ref.at[sl], hid.at[sl], lsem.at[i])

    def r_copy(i):
        sl = slice(i * part, (i + 1) * part)
        return pltpu.make_async_copy(r.at[sl], r_out.at[sl], lsem.at[n_part + i])

    w_copies = [
        pltpu.make_async_copy(wk_ref, wk, lsem.at[2 * n_part]),
        pltpu.make_async_copy(wv_ref, wv, lsem.at[2 * n_part + 1]),
    ]
    for i in range(n_part):
        hid_copy(i).start()
    for cpy in w_copies:
        cpy.start()

    pos = pos_ref[...]
    pos_row = jnp.concatenate([pos[t : t + 1] for t in range(pos.shape[0])], axis=1)
    angles = position_columns(pos_row.astype(jnp.float32)) * freq_ref[...]
    lane = lax.broadcasted_iota(jnp.int32, angles.shape, 1)
    sines = jnp.sin(angles)
    cos_ref[...] = jnp.cos(angles)
    sin_ref[...] = jnp.where(lane < HEAD // 2, -sines, sines)
    hi = jnp.broadcast_to((pos_row // POS_BASE).astype(jnp.float32), (POS_ROWS // 2, rows))
    lo = jnp.broadcast_to(lax.rem(pos_row, POS_BASE).astype(jnp.float32), (POS_ROWS // 2, rows))
    kv_ref[rows:, :] = jnp.concatenate([hi, lo], axis=0).astype(jnp.bfloat16)

    for i in range(n_part):
        sl = slice(i * part, (i + 1) * part)
        hid_copy(i).wait()
        x = hid[sl, :].astype(jnp.float32)
        scaled = x * lax.rsqrt(jnp.mean(x * x, axis=-1, keepdims=True) + EPS)
        r[sl, :] = (scaled * gain_ref[...]).astype(jnp.bfloat16)
        r_copy(i).start()
        if i == 0:
            for cpy in w_copies:
                cpy.wait()
        k = jnp.dot(r[sl, :], wk[...], preferred_element_type=jnp.float32)
        v = jnp.dot(r[sl, :], wv[...], preferred_element_type=jnp.float32).astype(jnp.bfloat16)
        kv_ref[sl, kv_cols:] = v
        rots = []
        for h in range(kv_cols // HEAD):
            cols = slice(h * HEAD, (h + 1) * HEAD)
            rot = rope(k[:, cols], cos_ref[sl, :], sin_ref[sl, :])
            kv_ref[sl, cols] = rot
            rots.append(rot)
        kc_ref[sl] = jnp.stack(rots, axis=1)
        vc_ref[sl] = jnp.stack([v[:, h * HEAD : (h + 1) * HEAD] for h in range(kv_cols // HEAD)], axis=1)
    for i in range(n_part):
        r_copy(i).wait()


def norm_kv(pos, freq, gain, hidden, wk, wv):
    rows, width = hidden.shape
    kv_cols = wk.shape[1]
    bf16, f32 = jnp.bfloat16, jnp.float32
    cache = jax.ShapeDtypeStruct((rows, kv_cols // HEAD, HEAD), bf16)
    table = jax.ShapeDtypeStruct((rows, HEAD), f32)
    return pl.pallas_call(
        norm_kv_kernel,
        in_specs=[vmem_spec()] * 3 + [any_spec()] * 3,
        out_specs=[any_spec()] + [vmem_spec()] * 5,
        out_shape=[
            jax.ShapeDtypeStruct((rows, width), bf16),
            jax.ShapeDtypeStruct((rows + POS_ROWS, 2 * kv_cols), bf16),
            table, table, cache, cache,
        ],
        scratch_shapes=[
            pltpu.VMEM((rows, width), bf16),
            pltpu.VMEM(wk.shape, bf16),
            pltpu.VMEM(wv.shape, bf16),
            pltpu.VMEM((rows, width), bf16),
            pltpu.SemaphoreType.DMA((8,)),
        ],
        compiler_params=pltpu.CompilerParams(vmem_limit_bytes=VMEM_LIMIT),
        name="norm_kv",
    )(pos, freq, gain, hidden, wk, wv)


def copy_kernel(src, dst, buf, isem, osem):
    n = buf.shape[0]
    tile = src.shape[0] // n
    def load(i):
        return pltpu.make_async_copy(src.at[pl.ds(i * tile, tile)], buf.at[i], isem.at[i])
    def store(i):
        return pltpu.make_async_copy(buf.at[i], dst.at[pl.ds(i * tile, tile)], osem.at[i])
    for i in range(n):
        load(i).start()
    for i in range(n):
        load(i).wait()
        store(i).start()
    for i in range(n):
        store(i).wait()


def copy_out(arr):
    n = 8
    rows, width = arr.shape
    return pl.pallas_call(
        copy_kernel,
        in_specs=[any_spec()],
        out_specs=any_spec(),
        out_shape=jax.ShapeDtypeStruct(arr.shape, arr.dtype),
        scratch_shapes=[
            pltpu.VMEM((n, rows // n, width), arr.dtype),
            pltpu.SemaphoreType.DMA((n,)),
            pltpu.SemaphoreType.DMA((n,)),
        ],
        name="copy_out",
    )(arr)


def block_kernel(
    n_tp, n_x, kv_ref, r_hbm, cos_hbm, sin_hbm, wq_ref, wo_ref, hid_ref, out_hbm,
    kv, r_ref, cos_ref, sin_ref, wq, wf, ct, q, mx, ls, acc, hs, pos_q_ref, out_ref, ssem, rsem, lsem,
):
    rows, width = r_ref.shape
    heads = wq_ref.shape[1] // HEAD
    kv_heads = mx.shape[1]
    group = heads // kv_heads
    kv_cols = kv_heads * HEAD
    n_chunk, chunk = mx.shape[0], mx.shape[2] // group
    ctx_cols = heads * HEAD
    cols = width // n_tp
    half = rows // 2
    tp, cp = lax.axis_index("tp"), lax.axis_index("cp")
    x, core = cp // 2, cp % 2

    def at_x(dx, dc=0):
        return lax.rem(x + dx + n_x, n_x) * 2 + lax.rem(core + dc, 2)

    def at_y(dy):
        return lax.rem(tp + dy + n_tp, n_tp)

    x_right, x_left, partner = {"cp": at_x(1)}, {"cp": at_x(-1)}, {"cp": at_x(0, 1)}
    y_right, y_left, y_far = {"tp": at_y(1)}, {"tp": at_y(-1)}, {"tp": at_y(2)}

    def rc(src, dst, idx, dev):
        return pltpu.make_async_remote_copy(
            src_ref=src, dst_ref=dst, send_sem=ssem.at[idx], recv_sem=rsem.at[idx], device_id=dev, device_id_type=MESH
        )

    barrier = pltpu.get_barrier_semaphore()
    peers = (x_right, x_left, partner, y_right, y_left, y_far)
    for dev in peers:
        pl.semaphore_signal(barrier, inc=1, device_id=dev, device_id_type=MESH)
    pl.semaphore_wait(barrier, len(peers))

    top, low = pl.ds(0, half), pl.ds(half, half + POS_ROWS)
    kv_copies = [
        rc(kv_ref.at[top], kv.at[2, top], 0, x_right),
        rc(kv_ref.at[low], kv.at[3, low], 1, x_left),
        rc(kv_ref.at[low], kv.at[2, low], 2, x_right),
        rc(kv_ref.at[top], kv.at[3, top], 3, x_left),
        rc(kv_ref, kv.at[1], 4, partner),
        rc(kv.at[2, top], kv.at[6, top], 5, x_right),
        rc(kv.at[3, low], kv.at[6, low], 6, x_left),
        rc(kv.at[2], kv.at[4], 7, partner),
        rc(kv.at[3], kv.at[5], 8, partner),
        rc(kv.at[6], kv.at[7], 9, partner),
    ]
    for cpy in kv_copies[:5]:
        cpy.start()

    piece = wf.shape[1] // (2 * n_x)

    def w_rows(idx, part=None):
        if part is None:
            return pl.ds(pl.multiple_of(idx * piece, piece), piece)
        return pl.ds(pl.multiple_of(idx * piece + part * (piece // 2), piece // 2), piece // 2)

    def w_cols(t):
        return pl.ds(pl.multiple_of(t * cols, cols), cols)

    mine = w_rows(cp)
    w_swap = [
        rc(wo_ref.at[mine, w_cols(at_y(1))], wf.at[1, mine], 10, y_right),
        rc(wo_ref.at[mine, w_cols(at_y(-1))], wf.at[2, mine], 11, y_left),
        rc(wo_ref.at[mine, w_cols(at_y(2))], wf.at[3, mine], 12, y_far),
    ]
    for cpy in w_swap:
        cpy.start()

    n_q = 4
    q_cols = ctx_cols // n_q

    def wq_copy(c):
        sl = pl.ds(pl.multiple_of(c * q_cols, q_cols), q_cols)
        return pltpu.make_async_copy(wq_ref.at[:, sl], wq.at[c], lsem.at[c])

    local = [
        pltpu.make_async_copy(cos_hbm, cos_ref, lsem.at[n_q]),
        pltpu.make_async_copy(sin_hbm, sin_ref, lsem.at[n_q + 1]),
        pltpu.make_async_copy(r_hbm, r_ref, lsem.at[n_q + 2]),
        pltpu.make_async_copy(kv_ref, kv.at[0], lsem.at[n_q + 3]),
        pltpu.make_async_copy(wo_ref.at[:, w_cols(tp)], wf.at[0], lsem.at[n_q + 4]),
        pltpu.make_async_copy(hid_ref.at[:, w_cols(tp)], hs, lsem.at[n_q + 5]),
    ]
    for cpy in local[:3]:
        cpy.start()
    for c in range(n_q):
        wq_copy(c).start()
    for cpy in local[3:]:
        cpy.start()
    for cpy in local[:3]:
        cpy.wait()

    @pl.loop(0, n_q)
    def _(c):
        wq_copy(c).wait()
        qc = jnp.dot(r_ref[...], wq[c], preferred_element_type=jnp.float32)
        per = q_cols // HEAD
        for j in range(per):
            rot = rope(qc[:, j * HEAD : (j + 1) * HEAD], cos_ref[...], sin_ref[...])
            head = c * per + j
            kvh, g = head // group, lax.rem(head, group)
            for i in range(n_chunk):
                q[i, kvh, pl.ds(pl.multiple_of(g * chunk, chunk), chunk), :] = rot[i * chunk : (i + 1) * chunk]

    mx[...] = jnp.full_like(mx, NEG_BIG)
    ls[...] = jnp.zeros_like(ls)
    acc[...] = jnp.zeros_like(acc)
    scale = HEAD**-0.5 * LOG2E

    def block_positions(slot):
        hi = kv[slot, pl.ds(rows, POS_ROWS // 2), :].astype(jnp.float32)
        lo = kv[slot, pl.ds(rows + POS_ROWS // 2, POS_ROWS // 2), :].astype(jnp.float32)
        return (hi * POS_BASE + lo)[0:1, :]

    def attend(i, slot):
        pos_q = pos_q_ref[pl.ds(pl.multiple_of(i * chunk, chunk), chunk), :]
        pos_k = block_positions(slot)
        n_l = rows // HEAD
        bias = jnp.concatenate(
            [jnp.where(pos_k[:, t * HEAD : (t + 1) * HEAD] <= pos_q, 0.0, NEG_BIG) for t in range(n_l)], axis=1
        )
        for kvh in range(kv_heads):
            k_blk = kv[slot, pl.ds(0, rows), kvh * HEAD : (kvh + 1) * HEAD]
            v_blk = kv[slot, pl.ds(0, rows), kv_cols + kvh * HEAD : kv_cols + (kvh + 1) * HEAD]
            s = lax.dot_general(q[i, kvh], k_blk, (((1,), (1,)), ((), ())), preferred_element_type=jnp.float32)
            s = (s.reshape(group, chunk, rows) * scale + bias[None]).reshape(group * chunk, rows)
            m_old = mx[i, kvh]
            m_new = jnp.maximum(m_old, jnp.max(s, axis=1, keepdims=True))
            alpha = jnp.exp2(m_old - m_new)
            p = jnp.exp2(s - jnp.concatenate([m_new] * n_l, axis=1))
            part = p[:, :HEAD]
            for t in range(1, n_l):
                part = part + p[:, t * HEAD : (t + 1) * HEAD]
            mx[i, kvh] = m_new
            ls[i, kvh] = ls[i, kvh] * alpha + part
            acc[i, kvh] = acc[i, kvh] * alpha + jnp.dot(
                p.astype(jnp.bfloat16), v_blk, preferred_element_type=jnp.float32
            )

    n_lead = n_chunk // 2

    def attend_pair(first):
        @pl.loop(0, 2 * n_lead)
        def _(t):
            attend(t // 2, first + lax.rem(t, 2))

    for cpy in local[3:]:
        cpy.wait()
    pos_q_ref[...] = position_columns(block_positions(0))
    kv_copies[0].wait_recv()
    kv_copies[5].start()
    kv_copies[1].wait_recv()
    kv_copies[6].start()
    kv_copies[4].wait_recv()
    attend_pair(0)

    for cpy in w_swap:
        cpy.wait_recv()

    def w_piece(idx, part=None):
        return wf.at[pl.ds(1, n_tp - 1), w_rows(idx, part)]

    own, right, left, far = cp, at_x(-1), at_x(1), at_x(2)

    def w_copy(src_idx, idx, dev, part=None):
        return rc(w_piece(src_idx, part), w_piece(src_idx, part), idx, dev)

    kv_copies[2].wait_recv()
    kv_copies[7].start()
    kv_copies[3].wait_recv()
    kv_copies[8].start()
    for idx, dev in ((13, x_right), (14, x_left), (15, partner)):
        w_copy(own, idx, dev).start()
    attend_pair(2)
    kv_copies[5].wait_recv()
    kv_copies[6].wait_recv()
    kv_copies[9].start()
    kv_copies[7].wait_recv()
    kv_copies[8].wait_recv()
    attend_pair(4)
    kv_copies[9].wait_recv()

    base = 24
    hc = chunk // 2

    def rows_of(i, part=None):
        if part is None:
            return pl.ds(pl.multiple_of(i * chunk, chunk), chunk)
        return pl.ds(pl.multiple_of(i * chunk + part * hc, hc), hc)

    def ctx_copies(i):
        sl = rows_of(i)
        first, second = rows_of(i, 0), rows_of(i, 1)
        b = base + 4 * i
        return (
            rc(ct.at[0, sl], ct.at[1, sl], b, y_right),
            rc(ct.at[0, sl], ct.at[2, sl], b + 1, y_left),
            rc(ct.at[1, first], ct.at[3, first], b + 2, y_right),
            rc(ct.at[2, second], ct.at[3, second], b + 3, y_left),
        )

    def finish(i):
        for kvh in range(kv_heads):
            total = jnp.sum(ls[i, kvh], axis=1, keepdims=True)
            ctx = (acc[i, kvh] / total).astype(jnp.bfloat16)
            for g in range(group):
                h = kvh * group + g
                ct[0, rows_of(i), h * HEAD : (h + 1) * HEAD] = ctx[g * chunk : (g + 1) * chunk]
        to_right, to_left, _, _ = ctx_copies(i)
        to_right.start()
        to_left.start()

    def ctx_forward(i):
        to_right, to_left, fwd_right, fwd_left = ctx_copies(i)
        to_right.wait_recv()
        fwd_right.start()
        to_left.wait_recv()
        fwd_left.start()

    @pl.loop(0, n_lead)
    def _(i):
        attend(i, 6)
        attend(i, 7)
        finish(i)

    @pl.loop(n_lead, n_chunk)
    def _(i):
        @pl.loop(0, 2 * n_x)
        def _(slot):
            attend(i, slot)

        finish(i)
        ctx_forward(i - n_lead)

    w_copy(right, 13, x_right).wait_recv()
    w_copy(right, 16, x_right, 0).start()
    w_copy(right, 18, partner).start()
    w_copy(left, 14, x_left).wait_recv()
    w_copy(left, 17, x_left, 1).start()
    w_copy(left, 19, partner).start()
    ctx_forward(2)
    w_copy(far, 16, x_right, 0).wait_recv()
    w_copy(far, 17, x_left, 1).wait_recv()
    w_copy(far, 20, partner).start()
    ctx_forward(3)
    for idx, src in ((15, own), (18, right), (19, left), (20, far)):
        w_copy(src, idx, partner).wait_recv()

    out_base = base + 4 * n_chunk

    def out_copies(i):
        sl, first, second = rows_of(i), rows_of(i, 0), rows_of(i, 1)
        b = out_base + 4 * i
        mine_c, right_c, left_c = w_cols(tp), w_cols(at_y(-1)), w_cols(at_y(1))
        return (
            rc(out_ref.at[sl, mine_c], out_ref.at[sl, mine_c], b, y_right),
            rc(out_ref.at[sl, mine_c], out_ref.at[sl, mine_c], b + 1, y_left),
            rc(out_ref.at[first, right_c], out_ref.at[first, right_c], b + 2, y_right),
            rc(out_ref.at[second, left_c], out_ref.at[second, left_c], b + 3, y_left),
        )

    @pl.loop(0, n_chunk)
    def _(i):
        _, _, fwd_right, fwd_left = ctx_copies(i)
        fwd_right.wait_recv()
        fwd_left.wait_recv()
        sl = rows_of(i)
        y = hs[sl, :].astype(jnp.float32)
        proj = jnp.dot(ct[0, sl, :], wf[0], preferred_element_type=jnp.float32)
        for j in range(1, n_tp):
            proj = proj + jnp.dot(ct[j, sl, :], wf[j], preferred_element_type=jnp.float32)
        out_ref[sl, w_cols(tp)] = (y + proj).astype(jnp.bfloat16)
        to_right, to_left, _, _ = out_copies(i)
        to_right.start()
        to_left.start()

    @pl.loop(0, n_chunk)
    def _(i):
        to_right, to_left, fwd_right, fwd_left = out_copies(i)
        to_right.wait_recv()
        fwd_right.start()
        to_left.wait_recv()
        fwd_left.start()

    def out_store(i):
        return pltpu.make_async_copy(out_ref.at[rows_of(i)], out_hbm.at[rows_of(i)], lsem.at[i])

    for cpy in kv_copies + w_swap:
        cpy.wait_send()
    for src, idx, dev, part in (
        (own, 13, x_right, None), (own, 14, x_left, None), (own, 15, partner, None), (right, 16, x_right, 0),
        (left, 17, x_left, 1), (right, 18, partner, None), (left, 19, partner, None), (far, 20, partner, None),
    ):
        w_copy(src, idx, dev, part).wait_send()

    @pl.loop(0, n_chunk)
    def _(i):
        for cpy in ctx_copies(i):
            cpy.wait_send()
        for cpy in out_copies(i):
            cpy.wait_send()
        _, _, fwd_right, fwd_left = out_copies(i)
        fwd_right.wait_recv()
        fwd_left.wait_recv()
        out_store(i).start()

    @pl.loop(0, n_chunk)
    def _(i):
        out_store(i).wait()


def attention_block(mesh, kv_blk, normed, cos_full, sin_full, w_query, w_out, hidden):
    n_tp, n_x = mesh.shape["tp"], mesh.shape["cp"] // 2
    rows, width = hidden.shape
    heads = w_query.shape[1] // HEAD
    kv_heads = kv_blk.shape[1] // (2 * HEAD)
    n_chunk = 4
    chunk = rows // n_chunk
    grp = heads // kv_heads * chunk
    bf16, f32 = jnp.bfloat16, jnp.float32
    n_sem = 24 + 8 * n_chunk
    return pl.pallas_call(
        functools.partial(block_kernel, n_tp, n_x),
        out_shape=jax.ShapeDtypeStruct((rows, width), bf16),
        in_specs=[any_spec()] * 7,
        out_specs=any_spec(),
        scratch_shapes=[
            pltpu.VMEM((2 * n_x, *kv_blk.shape), bf16),
            pltpu.VMEM((rows, width), bf16),
            pltpu.VMEM((rows, HEAD), f32),
            pltpu.VMEM((rows, HEAD), f32),
            pltpu.VMEM((4, width, w_query.shape[1] // 4), bf16),
            pltpu.VMEM((n_tp, w_out.shape[0], width // n_tp), bf16),
            pltpu.VMEM((n_tp, rows, heads * HEAD), bf16),
            pltpu.VMEM((n_chunk, kv_heads, grp, HEAD), bf16),
            pltpu.VMEM((n_chunk, kv_heads, grp, HEAD), f32),
            pltpu.VMEM((n_chunk, kv_heads, grp, HEAD), f32),
            pltpu.VMEM((n_chunk, kv_heads, grp, HEAD), f32),
            pltpu.VMEM((rows, width // n_tp), bf16),
            pltpu.VMEM((rows, HEAD), f32),
            pltpu.VMEM((rows, width), bf16),
            pltpu.SemaphoreType.DMA((n_sem,)),
            pltpu.SemaphoreType.DMA((n_sem,)),
            pltpu.SemaphoreType.DMA((16,)),
        ],
        compiler_params=pltpu.CompilerParams(collective_id=0, has_side_effects=True, vmem_limit_bytes=VMEM_LIMIT),
        name="attention_block",
    )(kv_blk, normed, cos_full, sin_full, w_query, w_out, hidden)


def solution(mesh):
    def local_block(hidden, tok_pos, norm_gain, w_query, w_key, w_value, w_out):
        normed, kv_blk, cos_full, sin_full, k_cache, v_cache = norm_kv(
            tok_pos.reshape(-1, HEAD), inv_freq_row(), norm_gain[None, :], hidden, w_key, w_value
        )
        hidden_out = attention_block(mesh, kv_blk, normed, cos_full, sin_full, w_query, w_out, hidden)
        return copy_out(hidden_out), k_cache, v_cache

    row_spec = P(("dp", "cp"), None)
    cache_spec = P(("dp", "cp"), "tp", None)
    return jax.shard_map(
        local_block,
        mesh=mesh,
        in_specs=(row_spec, P(("dp", "cp")), P(None), P(None, "tp"), P(None, "tp"), P(None, "tp"), P("tp", None)),
        out_specs=(row_spec, cache_spec, cache_spec),
        check_vma=False,
    )
```

```python
import functools

import jax
import jax.numpy as jnp
from jax import lax
from jax.experimental import pallas as pl
from jax.experimental.pallas import tpu as pltpu
from jax.sharding import PartitionSpec as P

HEAD = 128
THETA = 1000000
EPS = 1e-5
NEG_BIG = -1e30
LOG2E = 1.4426950408889634
MESH = pl.DeviceIdType.MESH
VMEM_LIMIT = 64 * 2**20 - 64 * 2**10
POS_ROWS = 16
POS_BASE = 64
E_FRACTION = (3, 8)
N_Q = 4


def vmem_spec():
    return pl.BlockSpec(memory_space=pltpu.VMEM)


def any_spec():
    return pl.BlockSpec(memory_space=pl.ANY)


def inv_freq_row():
    freq = 1.0 / (THETA ** (jnp.arange(0, HEAD, 2, dtype=jnp.float32) / HEAD))
    return jnp.concatenate([freq, freq])[None, :]


def rope(head_f32, cos_full, sin_full):
    vals = head_f32.astype(jnp.bfloat16).astype(jnp.float32)
    return (vals * cos_full + pltpu.roll(vals, HEAD // 2, 1) * sin_full).astype(jnp.bfloat16)


def position_columns(pos_row):
    tiles = []
    for t in range(pos_row.shape[1] // HEAD):
        tile = jnp.broadcast_to(pos_row[:, t * HEAD : (t + 1) * HEAD], (HEAD, HEAD))
        tiles.append(jnp.transpose(tile))
    return jnp.concatenate(tiles, axis=0)


def block_kernel(
    n_tp, n_x, pos_ref, freq_ref, gain_ref, hid_hbm, wk_hbm, wv_hbm, wq_hbm, wo_hbm, out_hbm, kc_hbm, vc_hbm,
    kv, r, cos, sin, wq, wr, we, ct, q, mx, ls, acc, acc_e, pos_q, out, kc, vc, ssem, rsem, lsem,
):
    rows, width = r.shape
    kv_cols = wk_hbm.shape[1]
    kv_heads = kv_cols // HEAD
    heads = wq_hbm.shape[1] // HEAD
    group = heads // kv_heads
    n_chunk, chunk = mx.shape[0], mx.shape[2] // group
    n_cp = 2 * n_x
    half = rows // 2
    cols = wr.shape[2]
    e_cols = we.shape[3]
    piece = we.shape[2]
    q_cols = wq.shape[2]
    tp, cp = lax.axis_index("tp"), lax.axis_index("cp")
    x, core = cp // 2, cp % 2

    def at_x(dx, dc=0):
        return lax.rem(x + dx + n_x, n_x) * 2 + lax.rem(core + dc, 2)

    def at_y(dy):
        return lax.rem(tp + dy + n_tp, n_tp)

    x_right, x_left, partner = {"cp": at_x(1)}, {"cp": at_x(-1)}, {"cp": at_x(0, 1)}
    y_right, y_left, y_far = {"tp": at_y(1)}, {"tp": at_y(-1)}, {"tp": at_y(2)}

    def rc(src, dst, idx, dev):
        return pltpu.make_async_remote_copy(
            src_ref=src, dst_ref=dst, send_sem=ssem.at[idx], recv_sem=rsem.at[idx], device_id=dev, device_id_type=MESH
        )

    def lc(src, dst, idx):
        return pltpu.make_async_copy(src, dst, lsem.at[idx])

    def part_of(i, size, sub=None):
        if sub is None:
            return pl.ds(pl.multiple_of(i * size, size), size)
        return pl.ds(pl.multiple_of(i * size + sub * (size // 2), size // 2), size // 2)

    halves = (slice(0, half), slice(half, rows))
    r_cols = lambda t: pl.ds(pl.multiple_of(e_cols + t * cols, HEAD), cols)
    hid_copy = lambda i: lc(hid_hbm.at[halves[i]], out.at[halves[i]], i)
    wk_copy = lambda: lc(wk_hbm, wq.at[N_Q - 2], 2)
    wv_copy = lambda: lc(wv_hbm, wq.at[N_Q - 1], 3)
    wq_copy = lambda c: lc(wq_hbm.at[:, part_of(c, q_cols)], wq.at[c], 4 + c)
    wr_copy = lambda: lc(wo_hbm.at[:, r_cols(tp)], wr.at[0], 4 + N_Q)
    kc_copy = lambda: lc(kc, kc_hbm, 5 + N_Q)
    vc_copy = lambda: lc(vc, vc_hbm, 6 + N_Q)
    we_copy = lambda j: lc(wo_hbm.at[part_of(j, piece), pl.ds(0, e_cols)], we.at[j, 0], 7 + N_Q + j)
    out_copy = lambda i: lc(out.at[part_of(i, chunk)], out_hbm.at[part_of(i, chunk)], 7 + N_Q + n_cp + i)

    top, low = pl.ds(0, half), pl.ds(half, half + POS_ROWS)

    def kv_copy(k):
        src, dst, dev = (
            ((0, top), (2, top), x_right),
            ((0, top), (3, top), x_left),
            ((0, low), (3, low), x_left),
            ((0, low), (2, low), x_right),
            ((0,), (1,), partner),
            ((2, top), (6, top), x_right),
            ((3, low), (6, low), x_left),
            ((2,), (4,), partner),
            ((3,), (5,), partner),
            ((6,), (7,), partner),
        )[k]
        return rc(kv.at[src], kv.at[dst], k, dev)

    y_devs = (y_right, y_left, y_far)
    mine = part_of(cp, piece)

    def wr_swap(k):
        return rc(wo_hbm.at[mine, r_cols(at_y((1, -1, 2)[k]))], wr.at[1 + k, mine], 10 + k, y_devs[k])

    def we_swap(k):
        return rc(wo_hbm.at[mine, pl.ds(0, e_cols)], we.at[cp, 1 + k], 13 + k, y_devs[k])

    own, right, left, far = cp, at_x(-1), at_x(1), at_x(2)
    ring = (
        (own, x_right, None), (own, x_left, None), (own, partner, None), (right, x_right, 0), (left, x_left, 1),
        (right, partner, None), (left, partner, None), (far, partner, None),
    )

    def wr_ring(m):
        src, dev, sub = ring[m]
        ref = wr.at[pl.ds(1, n_tp - 1), part_of(src, piece, sub)]
        return rc(ref, ref, 16 + m, dev)

    def we_ring(k, m):
        src, dev, sub = ring[m]
        ref = we.at[src, k] if sub is None else we.at[src, k, part_of(sub, piece // 2)]
        return rc(ref, ref, 16 + 8 * k + m, dev)

    def start_own(copy):
        for m in range(3):
            copy(m).start()

    def pass_on(copy):
        copy(0).wait_recv()
        copy(3).start()
        copy(5).start()
        copy(1).wait_recv()
        copy(4).start()
        copy(6).start()

    def pass_far(copy):
        copy(3).wait_recv()
        copy(4).wait_recv()
        copy(7).start()

    ctx_base = 16 + 8 * n_tp
    out_base = ctx_base + 4 * n_chunk

    def ctx_copy(i, k):
        src, dst, sub, dev = ((0, 1, None, y_right), (0, 2, None, y_left), (1, 3, 0, y_right), (2, 3, 1, y_left))[k]
        sl = part_of(i, chunk, sub)
        return rc(ct.at[src, sl], ct.at[dst, sl], ctx_base + 4 * i + k, dev)

    def res_copy(i, k):
        t, sub, dev = ((tp, None, y_right), (tp, None, y_left), (at_y(-1), 0, y_right), (at_y(1), 1, y_left))[k]
        ref = out.at[part_of(i, chunk, sub), r_cols(t)]
        return rc(ref, ref, out_base + 4 * i + k, dev)

    def forward(copy, i):
        copy(i, 0).wait_recv()
        copy(i, 2).start()
        copy(i, 1).wait_recv()
        copy(i, 3).start()

    barrier = pltpu.get_barrier_semaphore()
    peers = (x_right, x_left, partner) + y_devs
    for dev in peers:
        pl.semaphore_signal(barrier, inc=1, device_id=dev, device_id_type=MESH)
    hid_copy(0).start()
    wk_copy().start()
    wv_copy().start()
    hid_copy(1).start()
    for c in range(N_Q - 2):
        wq_copy(c).start()

    pos = pos_ref[...]
    pos_row = jnp.concatenate([pos[t : t + 1] for t in range(pos.shape[0])], axis=1)
    pos_q[...] = position_columns(pos_row.astype(jnp.float32))
    angles = pos_q[...] * freq_ref[...]
    lane = lax.broadcasted_iota(jnp.int32, angles.shape, 1)
    sines = jnp.sin(angles)
    cos[...] = jnp.cos(angles)
    sin[...] = jnp.where(lane < HEAD // 2, -sines, sines)
    hi = jnp.broadcast_to((pos_row // POS_BASE).astype(jnp.float32), (POS_ROWS // 2, rows))
    lo = jnp.broadcast_to(lax.rem(pos_row, POS_BASE).astype(jnp.float32), (POS_ROWS // 2, rows))
    kv[0, rows:, :] = jnp.concatenate([hi, lo], axis=0).astype(jnp.bfloat16)

    pl.semaphore_wait(barrier, len(peers))
    for k in range(n_tp - 1):
        wr_swap(k).start()
    for k in range(n_tp - 1):
        we_swap(k).start()

    for i, sl in enumerate(halves):
        hid_copy(i).wait()
        hid = out[sl, :].astype(jnp.float32)
        scaled = hid * lax.rsqrt(jnp.mean(hid * hid, axis=-1, keepdims=True) + EPS)
        r[sl, :] = (scaled * gain_ref[...]).astype(jnp.bfloat16)
        if i == 0:
            wk_copy().wait()
            wv_copy().wait()
        k = jnp.dot(r[sl, :], wq[N_Q - 2], preferred_element_type=jnp.float32)
        v = jnp.dot(r[sl, :], wq[N_Q - 1], preferred_element_type=jnp.float32).astype(jnp.bfloat16)
        kv[0, sl, kv_cols:] = v
        rots = []
        for h in range(kv_heads):
            rots.append(rope(k[:, h * HEAD : (h + 1) * HEAD], cos[sl, :], sin[sl, :]))
            kv[0, sl, h * HEAD : (h + 1) * HEAD] = rots[h]
        if i == 0:
            kv_copy(0).start()
            kv_copy(1).start()
        else:
            kv_copy(2).start()
            kv_copy(3).start()
            kv_copy(4).start()
        kc[sl] = jnp.stack(rots, axis=1)
        vc[sl] = jnp.stack([v[:, h * HEAD : (h + 1) * HEAD] for h in range(kv_heads)], axis=1)
    for c in range(N_Q - 2, N_Q):
        wq_copy(c).start()
    kc_copy().start()
    vc_copy().start()
    wr_copy().start()
    for j in range(n_cp):
        we_copy(j).start()

    @pl.loop(0, N_Q)
    def _(c):
        wq_copy(c).wait()
        qc = jnp.dot(r[...], wq[c], preferred_element_type=jnp.float32)
        per = q_cols // HEAD
        for j in range(per):
            rot = rope(qc[:, j * HEAD : (j + 1) * HEAD], cos[...], sin[...])
            head = c * per + j
            kvh, g = head // group, lax.rem(head, group)
            for i in range(n_chunk):
                q[i, kvh, part_of(g, chunk), :] = rot[i * chunk : (i + 1) * chunk]

    mx[...] = jnp.full_like(mx, NEG_BIG)
    ls[...] = jnp.zeros_like(ls)
    acc[...] = jnp.zeros_like(acc)
    scale = HEAD**-0.5 * LOG2E

    def attend(i, slot):
        hi = kv[slot, pl.ds(rows, POS_ROWS // 2), :].astype(jnp.float32)
        lo = kv[slot, pl.ds(rows + POS_ROWS // 2, POS_ROWS // 2), :].astype(jnp.float32)
        pos_k = (hi * POS_BASE + lo)[0:1, :]
        pos_i = pos_q[part_of(i, chunk), :]
        n_l = rows // HEAD
        bias = jnp.concatenate(
            [jnp.where(pos_k[:, t * HEAD : (t + 1) * HEAD] <= pos_i, 0.0, NEG_BIG) for t in range(n_l)], axis=1
        )
        for kvh in range(kv_heads):
            k_blk = kv[slot, pl.ds(0, rows), kvh * HEAD : (kvh + 1) * HEAD]
            v_blk = kv[slot, pl.ds(0, rows), kv_cols + kvh * HEAD : kv_cols + (kvh + 1) * HEAD]
            s = lax.dot_general(q[i, kvh], k_blk, (((1,), (1,)), ((), ())), preferred_element_type=jnp.float32)
            s = (s.reshape(group, chunk, rows) * scale + bias[None]).reshape(group * chunk, rows)
            m_old = mx[i, kvh]
            m_new = jnp.maximum(m_old, jnp.max(s, axis=1, keepdims=True))
            alpha = jnp.exp2(m_old - m_new)
            p = jnp.exp2(s - jnp.concatenate([m_new] * n_l, axis=1))
            part = p[:, :HEAD]
            for t in range(1, n_l):
                part = part + p[:, t * HEAD : (t + 1) * HEAD]
            mx[i, kvh] = m_new
            ls[i, kvh] = ls[i, kvh] * alpha + part
            acc[i, kvh] = acc[i, kvh] * alpha + jnp.dot(
                p.astype(jnp.bfloat16), v_blk, preferred_element_type=jnp.float32
            )

    n_lead = n_chunk // 2

    def attend_pair(first):
        @pl.loop(0, 2 * n_lead)
        def _(t):
            attend(t // 2, first + lax.rem(t, 2))

    def finish(i):
        for kvh in range(kv_heads):
            total = jnp.sum(ls[i, kvh], axis=1, keepdims=True)
            ctx = (acc[i, kvh] / total).astype(jnp.bfloat16)
            for g in range(group):
                h = kvh * group + g
                ct[0, part_of(i, chunk), h * HEAD : (h + 1) * HEAD] = ctx[g * chunk : (g + 1) * chunk]
        ctx_copy(i, 0).start()
        ctx_copy(i, 1).start()

    kv_copy(0).wait_recv()
    kv_copy(5).start()
    kv_copy(2).wait_recv()
    kv_copy(6).start()
    kv_copy(4).wait_recv()
    attend_pair(0)
    for k in range(n_tp - 1):
        wr_swap(k).wait_recv()
    kv_copy(1).wait_recv()
    kv_copy(3).wait_recv()
    kv_copy(7).start()
    kv_copy(8).start()
    start_own(wr_ring)
    attend_pair(2)
    kv_copy(5).wait_recv()
    kv_copy(6).wait_recv()
    kv_copy(9).start()
    kv_copy(7).wait_recv()
    kv_copy(8).wait_recv()
    attend_pair(4)
    kv_copy(9).wait_recv()

    @pl.loop(0, n_lead)
    def _(i):
        attend(i, 6)
        attend(i, 7)
        finish(i)

    we_k = lambda k: functools.partial(we_ring, k)
    for k in range(n_tp - 1):
        we_swap(k).wait_recv()
    start_own(we_k(1))

    def late_chunk(i):
        @pl.loop(0, n_cp)
        def _(slot):
            attend(i, slot)

        finish(i)
        forward(ctx_copy, i - n_lead)

    late_chunk(n_lead)
    pass_on(wr_ring)
    for k in range(2, n_tp):
        start_own(we_k(k))
    late_chunk(n_lead + 1)
    pass_on(we_k(1))
    forward(ctx_copy, n_lead)
    pass_far(wr_ring)
    pass_on(we_k(2))
    forward(ctx_copy, n_lead + 1)
    for m in (2, 5, 6, 7):
        wr_ring(m).wait_recv()
    wr_copy().wait()

    @pl.loop(0, n_chunk)
    def _(i):
        ctx_copy(i, 2).wait_recv()
        ctx_copy(i, 3).wait_recv()
        sl = part_of(i, chunk)
        proj = jnp.dot(ct[0, sl, :], wr[0], preferred_element_type=jnp.float32)
        for t in range(1, n_tp):
            proj = proj + jnp.dot(ct[t, sl, :], wr[t], preferred_element_type=jnp.float32)
        out[sl, r_cols(tp)] = (out[sl, r_cols(tp)].astype(jnp.float32) + proj).astype(jnp.bfloat16)
        res_copy(i, 0).start()
        res_copy(i, 1).start()

    e_tile = 512
    n_e = e_cols // e_tile

    def project(j, first=False, last=False):
        ctx = jnp.concatenate([ct[t, :, part_of(j, piece)] for t in range(n_tp)], axis=1)

        @pl.loop(0, n_e)
        def _(n):
            sl = part_of(n, e_tile)
            w = we[j, :, :, sl].reshape(n_tp * piece, e_tile)
            add = jnp.dot(ctx, w, preferred_element_type=jnp.float32)
            if not first:
                add = acc_e[:, sl] + add
            if last:
                out[:, sl] = (out[:, sl].astype(jnp.float32) + add).astype(jnp.bfloat16)
            else:
                acc_e[:, sl] = add

    for j in range(n_cp):
        we_copy(j).wait()
    pass_on(we_k(3))
    project(own, first=True)
    forward(res_copy, 0)
    for k in range(1, n_tp):
        we_k(k)(2).wait_recv()
    project(at_x(0, 1))
    project(right)
    forward(res_copy, 1)
    project(left)
    forward(res_copy, 2)
    for k in range(1, n_tp):
        we_k(k)(5).wait_recv()
    project(at_x(-1, 1))
    for k in range(1, n_tp):
        we_k(k)(6).wait_recv()
    forward(res_copy, 3)
    project(at_x(1, 1))
    for k in range(1, n_tp):
        pass_far(we_k(k))
    project(far)
    for k in range(1, n_tp):
        we_k(k)(7).wait_recv()
    project(at_x(2, 1), last=True)

    @pl.loop(0, n_chunk)
    def _(i):
        res_copy(i, 2).wait_recv()
        res_copy(i, 3).wait_recv()
        out_copy(i).start()

    kc_copy().wait()
    vc_copy().wait()
    for k in range(10):
        kv_copy(k).wait_send()
    for k in range(n_tp - 1):
        wr_swap(k).wait_send()
        we_swap(k).wait_send()
    for m in range(8):
        wr_ring(m).wait_send()
        for k in range(1, n_tp):
            we_ring(k, m).wait_send()

    @pl.loop(0, n_chunk)
    def _(i):
        for k in range(4):
            ctx_copy(i, k).wait_send()
            res_copy(i, k).wait_send()
        out_copy(i).wait()


def attention_block(mesh, pos, freq, gain, hidden, w_key, w_value, w_query, w_out):
    n_tp, n_cp = mesh.shape["tp"], mesh.shape["cp"]
    rows, width = hidden.shape
    kv_cols = w_key.shape[1]
    heads, kv_heads = w_query.shape[1] // HEAD, kv_cols // HEAD
    n_chunk = 4
    grp = heads // kv_heads * (rows // n_chunk)
    e_cols = width * E_FRACTION[0] // E_FRACTION[1]
    cols = (width - e_cols) // n_tp
    k_rows = w_out.shape[0]
    bf16, f32 = jnp.bfloat16, jnp.float32
    n_sem = 16 + 8 * n_tp + 8 * n_chunk
    cache = (rows, kv_heads, HEAD)
    return pl.pallas_call(
        functools.partial(block_kernel, n_tp, n_cp // 2),
        out_shape=[jax.ShapeDtypeStruct(s, bf16) for s in ((rows, width), cache, cache)],
        in_specs=[vmem_spec()] * 3 + [any_spec()] * 5,
        out_specs=[any_spec()] * 3,
        scratch_shapes=[
            pltpu.VMEM((n_cp, rows + POS_ROWS, 2 * kv_cols), bf16),
            pltpu.VMEM((rows, width), bf16),
            pltpu.VMEM((rows, HEAD), f32),
            pltpu.VMEM((rows, HEAD), f32),
            pltpu.VMEM((N_Q, width, w_query.shape[1] // N_Q), bf16),
            pltpu.VMEM((n_tp, k_rows, cols), bf16),
            pltpu.VMEM((n_cp, n_tp, k_rows // n_cp, e_cols), bf16),
            pltpu.VMEM((n_tp, rows, k_rows), bf16),
            pltpu.VMEM((n_chunk, kv_heads, grp, HEAD), bf16),
            pltpu.VMEM((n_chunk, kv_heads, grp, HEAD), f32),
            pltpu.VMEM((n_chunk, kv_heads, grp, HEAD), f32),
            pltpu.VMEM((n_chunk, kv_heads, grp, HEAD), f32),
            pltpu.VMEM((rows, e_cols), f32),
            pltpu.VMEM((rows, HEAD), f32),
            pltpu.VMEM((rows, width), bf16),
            pltpu.VMEM(cache, bf16),
            pltpu.VMEM(cache, bf16),
            pltpu.SemaphoreType.DMA((n_sem,)),
            pltpu.SemaphoreType.DMA((n_sem,)),
            pltpu.SemaphoreType.DMA((32,)),
        ],
        compiler_params=pltpu.CompilerParams(collective_id=0, has_side_effects=True, vmem_limit_bytes=VMEM_LIMIT),
        name="attention_block",
    )(pos, freq, gain, hidden, w_key, w_value, w_query, w_out)


def copy_kernel(src, k_src, v_src, dst, k_dst, v_dst, buf, k_buf, v_buf, isem, osem):
    n = buf.shape[0]
    tile = src.shape[0] // n
    rows = lambda i: pl.ds(i * tile, tile)
    moves = [(src.at[rows(i)], buf.at[i], dst.at[rows(i)]) for i in range(n)]
    moves += [(k_src, k_buf, k_dst), (v_src, v_buf, v_dst)]
    for i, (a, b, _) in enumerate(moves):
        pltpu.make_async_copy(a, b, isem.at[i]).start()
    for i, (a, b, c) in enumerate(moves):
        pltpu.make_async_copy(a, b, isem.at[i]).wait()
        pltpu.make_async_copy(b, c, osem.at[i]).start()
    for i, (_, b, c) in enumerate(moves):
        pltpu.make_async_copy(b, c, osem.at[i]).wait()


def copy_out(*arrs):
    n = 8
    rows, width = arrs[0].shape
    return pl.pallas_call(
        copy_kernel,
        in_specs=[any_spec()] * 3,
        out_specs=[any_spec()] * 3,
        out_shape=[jax.ShapeDtypeStruct(a.shape, a.dtype) for a in arrs],
        scratch_shapes=[
            pltpu.VMEM((n, rows // n, width), arrs[0].dtype),
            *(pltpu.VMEM(a.shape, a.dtype) for a in arrs[1:]),
            pltpu.SemaphoreType.DMA((n + 2,)),
            pltpu.SemaphoreType.DMA((n + 2,)),
        ],
        name="copy_out",
    )(*arrs)


def solution(mesh):
    def local_block(hidden, tok_pos, norm_gain, w_query, w_key, w_value, w_out):
        results = attention_block(
            mesh, tok_pos.reshape(-1, HEAD), inv_freq_row(), norm_gain[None, :], hidden, w_key, w_value, w_query, w_out
        )
        return tuple(copy_out(*results))

    row_spec = P(("dp", "cp"), None)
    cache_spec = P(("dp", "cp"), "tp", None)
    return jax.shard_map(
        local_block,
        mesh=mesh,
        in_specs=(row_spec, P(("dp", "cp")), P(None), P(None, "tp"), P(None, "tp"), P(None, "tp"), P("tp", None)),
        out_specs=(row_spec, cache_spec, cache_spec),
        check_vma=False,
    )
```

```python
import functools

import jax
import jax.numpy as jnp
import numpy as np
from jax import lax
from jax.experimental import pallas as pl
from jax.experimental.pallas import tpu as pltpu
from jax.sharding import PartitionSpec as P

HEAD = 128
THETA = 1000000
EPS = 1e-5
NEG_BIG = -1e30
LOG2E = 1.4426950408889634
MESH = pl.DeviceIdType.MESH
VMEM_LIMIT = 64 * 2**20 - 64 * 2**10
POS_ROWS = 16
POS_BASE = 64
E_FRACTION = (3, 8)
N_Q = 4


def vmem_spec():
    return pl.BlockSpec(memory_space=pltpu.VMEM)


def any_spec():
    return pl.BlockSpec(memory_space=pl.ANY)


def inv_freq_row():
    freq = 1.0 / (np.float64(THETA) ** (np.arange(0, HEAD, 2) / HEAD))
    return jnp.asarray(np.concatenate([freq, freq])[None, :], jnp.float32)


def rope(head_f32, cos_full, sin_full):
    vals = head_f32.astype(jnp.bfloat16).astype(jnp.float32)
    return (vals * cos_full + pltpu.roll(vals, HEAD // 2, 1) * sin_full).astype(jnp.bfloat16)


def position_columns(pos_row):
    tiles = []
    for t in range(pos_row.shape[1] // HEAD):
        tile = jnp.broadcast_to(pos_row[:, t * HEAD : (t + 1) * HEAD], (HEAD, HEAD))
        tiles.append(jnp.transpose(tile))
    return jnp.concatenate(tiles, axis=0)


def block_kernel(
    n_tp, n_x, pos_ref, freq_ref, gain_ref, hid_hbm, wk_hbm, wv_hbm, wq_hbm, wo_hbm, out, kc, vc,
    kv, r, cos, sin, wq, wr, we, ct, q, mx, ls, acc, acc_e, pos_q, ssem, rsem, lsem,
):
    rows, width = r.shape
    kv_cols = wk_hbm.shape[1]
    kv_heads = kv_cols // HEAD
    heads = wq_hbm.shape[1] // HEAD
    group = heads // kv_heads
    n_chunk, chunk = mx.shape[0], mx.shape[2] // group
    n_cp = 2 * n_x
    n_ring = 18 + 8 * n_tp
    half = rows // 2
    cols = wr.shape[2]
    e_cols = we.shape[3]
    piece = we.shape[2]
    q_cols = wq.shape[2]
    tp, cp = lax.axis_index("tp"), lax.axis_index("cp")
    x, core = cp // 2, cp % 2

    def at_x(dx, dc=0):
        return lax.rem(x + dx + n_x, n_x) * 2 + lax.rem(core + dc, 2)

    def at_y(dy):
        return lax.rem(tp + dy + n_tp, n_tp)

    x_right, x_left, partner = {"cp": at_x(1)}, {"cp": at_x(-1)}, {"cp": at_x(0, 1)}
    y_right, y_left, y_far = {"tp": at_y(1)}, {"tp": at_y(-1)}, {"tp": at_y(2)}

    def rc(src, dst, idx, dev):
        return pltpu.make_async_remote_copy(
            src_ref=src, dst_ref=dst, send_sem=ssem.at[idx], recv_sem=rsem.at[idx], device_id=dev, device_id_type=MESH
        )

    def lc(src, dst, idx):
        return pltpu.make_async_copy(src, dst, lsem.at[idx])

    def part_of(i, size, sub=None):
        if sub is None:
            return pl.ds(pl.multiple_of(i * size, size), size)
        return pl.ds(pl.multiple_of(i * size + sub * (size // 2), size // 2), size // 2)

    quarter = half // 2
    parts = (slice(0, quarter), slice(quarter, half), slice(half, rows))
    r_cols = lambda t: pl.ds(pl.multiple_of(e_cols + t * cols, HEAD), cols)
    hid_copy = lambda i: lc(hid_hbm.at[parts[i]], out.at[parts[i]], i)
    wk_copy = lambda: lc(wk_hbm, wq.at[N_Q - 2], 3)
    wv_copy = lambda: lc(wv_hbm, wq.at[N_Q - 1], 4)
    wq_copy = lambda c: lc(wq_hbm.at[:, part_of(c, q_cols)], wq.at[c], 5 + c)
    wr_copy = lambda: lc(wo_hbm.at[:, r_cols(tp)], wr.at[0], 5 + N_Q)
    we_copy = lambda j: lc(wo_hbm.at[part_of(j, piece), pl.ds(0, e_cols)], we.at[j, 0], 6 + N_Q + j)

    top, low = pl.ds(0, half), pl.ds(half, half + POS_ROWS)
    top_a, top_b = pl.ds(0, quarter), pl.ds(quarter, quarter)

    def kv_copy(k):
        src, dst, dev = (
            ((0, top_a), (2, top_a), x_right),
            ((0, top_a), (3, top_a), x_left),
            ((0, low), (3, low), x_left),
            ((0, low), (2, low), x_right),
            ((0,), (1,), partner),
            ((2, top), (6, top), x_right),
            ((3, low), (6, low), x_left),
            ((2,), (4,), partner),
            ((3,), (5,), partner),
            ((6,), (7,), partner),
            ((0, top_b), (2, top_b), x_right),
            ((0, top_b), (3, top_b), x_left),
        )[k]
        return rc(kv.at[src], kv.at[dst], k if k < 10 else n_ring - 2 + k - 10, dev)

    y_devs = (y_right, y_left, y_far)
    mine = part_of(cp, piece)

    def wr_swap(k):
        return rc(wo_hbm.at[mine, r_cols(at_y((1, -1, 2)[k]))], wr.at[1 + k, mine], 10 + k, y_devs[k])

    def we_swap(k):
        return rc(wo_hbm.at[mine, pl.ds(0, e_cols)], we.at[cp, 1 + k], 13 + k, y_devs[k])

    own, right, left, far = cp, at_x(-1), at_x(1), at_x(2)
    ring = (
        (own, x_right, None), (own, x_left, None), (own, partner, None), (right, x_right, 0), (left, x_left, 1),
        (right, partner, None), (left, partner, None), (far, partner, None),
    )

    def wr_ring(m):
        src, dev, sub = ring[m]
        ref = wr.at[pl.ds(1, n_tp - 1), part_of(src, piece, sub)]
        return rc(ref, ref, 16 + m, dev)

    def we_ring(k, m):
        src, dev, sub = ring[m]
        ref = we.at[src, k] if sub is None else we.at[src, k, part_of(sub, piece // 2)]
        return rc(ref, ref, 16 + 8 * k + m, dev)

    def start_own(copy):
        for m in range(3):
            copy(m).start()

    def pass_on(copy):
        copy(0).wait_recv()
        copy(3).start()
        copy(5).start()
        copy(1).wait_recv()
        copy(4).start()
        copy(6).start()

    def pass_far(copy):
        copy(3).wait_recv()
        copy(4).wait_recv()
        copy(7).start()

    ctx_base = n_ring
    out_base = ctx_base + 4 * n_chunk

    def ctx_copy(i, k):
        src, dst, sub, dev = ((0, 1, None, y_right), (0, 2, None, y_left), (1, 3, 0, y_right), (2, 3, 1, y_left))[k]
        sl = part_of(i, chunk, sub)
        return rc(ct.at[src, sl], ct.at[dst, sl], ctx_base + 4 * i + k, dev)

    def res_copy(i, k):
        t, sub, dev = ((tp, None, y_right), (tp, None, y_left), (at_y(-1), 0, y_right), (at_y(1), 1, y_left))[k]
        ref = out.at[part_of(i, chunk, sub), r_cols(t)]
        return rc(ref, ref, out_base + 4 * i + k, dev)

    def forward(copy, i):
        copy(i, 0).wait_recv()
        copy(i, 2).start()
        copy(i, 1).wait_recv()
        copy(i, 3).start()

    barrier = pltpu.get_barrier_semaphore()
    peers = (x_right, x_left, partner) + y_devs
    for dev in peers:
        pl.semaphore_signal(barrier, inc=1, device_id=dev, device_id_type=MESH)
    hid_copy(0).start()
    wk_copy().start()
    wv_copy().start()
    hid_copy(1).start()
    hid_copy(2).start()
    for c in range(N_Q - 2):
        wq_copy(c).start()

    pos = pos_ref[...]
    pos_row = jnp.concatenate([pos[t : t + 1] for t in range(pos.shape[0])], axis=1)
    pos_q[...] = position_columns(pos_row.astype(jnp.float32))
    angles = pos_q[...] * freq_ref[...]
    lane = lax.broadcasted_iota(jnp.int32, angles.shape, 1)
    sines = jnp.sin(angles)
    cos[...] = jnp.cos(angles)
    sin[...] = jnp.where(lane < HEAD // 2, -sines, sines)
    hi = jnp.broadcast_to((pos_row // POS_BASE).astype(jnp.float32), (POS_ROWS // 2, rows))
    lo = jnp.broadcast_to(lax.rem(pos_row, POS_BASE).astype(jnp.float32), (POS_ROWS // 2, rows))
    kv[0, rows:, :] = jnp.concatenate([hi, lo], axis=0).astype(jnp.bfloat16)

    for i, sl in enumerate(parts):
        hid_copy(i).wait()
        hid = out[sl, :].astype(jnp.float32)
        scaled = hid * lax.rsqrt(jnp.mean(hid * hid, axis=-1, keepdims=True) + EPS)
        r[sl, :] = (scaled * gain_ref[...]).astype(jnp.bfloat16)
        if i == 0:
            wk_copy().wait()
            wv_copy().wait()
        k = jnp.dot(r[sl, :], wq[N_Q - 2], preferred_element_type=jnp.float32)
        v = jnp.dot(r[sl, :], wq[N_Q - 1], preferred_element_type=jnp.float32).astype(jnp.bfloat16)
        kv[0, sl, kv_cols:] = v
        rots = []
        for h in range(kv_heads):
            rots.append(rope(k[:, h * HEAD : (h + 1) * HEAD], cos[sl, :], sin[sl, :]))
            kv[0, sl, h * HEAD : (h + 1) * HEAD] = rots[h]
        if i == 0:
            pl.semaphore_wait(barrier, len(peers))
            kv_copy(0).start()
            kv_copy(1).start()
            for t in range(n_tp - 1):
                wr_swap(t).start()
            for t in range(n_tp - 1):
                we_swap(t).start()
        elif i == 1:
            kv_copy(10).start()
            kv_copy(11).start()
        else:
            kv_copy(2).start()
            kv_copy(3).start()
            kv_copy(4).start()
        kc[sl] = jnp.stack(rots, axis=1)
        vc[sl] = jnp.stack([v[:, h * HEAD : (h + 1) * HEAD] for h in range(kv_heads)], axis=1)
    for c in range(N_Q - 2, N_Q):
        wq_copy(c).start()
    wr_copy().start()
    for j in range(n_cp):
        we_copy(j).start()

    @pl.loop(0, N_Q)
    def _(c):
        wq_copy(c).wait()
        qc = jnp.dot(r[...], wq[c], preferred_element_type=jnp.float32)
        per = q_cols // HEAD
        for j in range(per):
            rot = rope(qc[:, j * HEAD : (j + 1) * HEAD], cos[...], sin[...])
            head = c * per + j
            kvh, g = head // group, lax.rem(head, group)
            for i in range(n_chunk):
                q[i, kvh, part_of(g, chunk), :] = rot[i * chunk : (i + 1) * chunk]

    mx[...] = jnp.full_like(mx, NEG_BIG)
    ls[...] = jnp.zeros_like(ls)
    acc[...] = jnp.zeros_like(acc)
    scale = HEAD**-0.5 * LOG2E

    def attend(i, slot):
        hi = kv[slot, pl.ds(rows, POS_ROWS // 2), :].astype(jnp.float32)
        lo = kv[slot, pl.ds(rows + POS_ROWS // 2, POS_ROWS // 2), :].astype(jnp.float32)
        pos_k = (hi * POS_BASE + lo)[0:1, :]
        pos_i = pos_q[part_of(i, chunk), :]
        n_l = rows // HEAD
        bias = jnp.concatenate(
            [jnp.where(pos_k[:, t * HEAD : (t + 1) * HEAD] <= pos_i, 0.0, NEG_BIG) for t in range(n_l)], axis=1
        )
        for kvh in range(kv_heads):
            k_blk = kv[slot, pl.ds(0, rows), kvh * HEAD : (kvh + 1) * HEAD]
            v_blk = kv[slot, pl.ds(0, rows), kv_cols + kvh * HEAD : kv_cols + (kvh + 1) * HEAD]
            s = lax.dot_general(q[i, kvh], k_blk, (((1,), (1,)), ((), ())), preferred_element_type=jnp.float32)
            s = (s.reshape(group, chunk, rows) * scale + bias[None]).reshape(group * chunk, rows)
            m_old = mx[i, kvh]
            m_new = jnp.maximum(m_old, jnp.max(s, axis=1, keepdims=True))
            alpha = jnp.exp2(m_old - m_new)
            p = jnp.exp2(s - jnp.concatenate([m_new] * n_l, axis=1))
            part = p[:, :HEAD]
            for t in range(1, n_l):
                part = part + p[:, t * HEAD : (t + 1) * HEAD]
            mx[i, kvh] = m_new
            ls[i, kvh] = ls[i, kvh] * alpha + part
            acc[i, kvh] = acc[i, kvh] * alpha + jnp.dot(
                p.astype(jnp.bfloat16), v_blk, preferred_element_type=jnp.float32
            )

    n_lead = n_chunk // 2

    def attend_all(chunks, first, n_slot):
        @pl.loop(0, (chunks[1] - chunks[0]) * n_slot)
        def _(t):
            attend(chunks[0] + t // n_slot, first + lax.rem(t, n_slot))

    def finish(i):
        for kvh in range(kv_heads):
            total = jnp.sum(ls[i, kvh], axis=1, keepdims=True)
            ctx = (acc[i, kvh] / total).astype(jnp.bfloat16)
            for g in range(group):
                h = kvh * group + g
                ct[0, part_of(i, chunk), h * HEAD : (h + 1) * HEAD] = ctx[g * chunk : (g + 1) * chunk]
        ctx_copy(i, 0).start()
        ctx_copy(i, 1).start()

    attend_all((0, 1), 0, 1)
    kv_copy(0).wait_recv()
    kv_copy(10).wait_recv()
    kv_copy(5).start()
    attend_all((1, n_lead), 0, 1)
    kv_copy(4).wait_recv()
    attend_all((0, n_lead), 1, 1)
    kv_copy(2).wait_recv()
    kv_copy(6).start()
    attend_all((n_lead, n_lead + 1), 0, 2)
    for t in range(n_tp - 1):
        wr_swap(t).wait_recv()
    kv_copy(1).wait_recv()
    kv_copy(11).wait_recv()
    kv_copy(3).wait_recv()
    kv_copy(7).start()
    kv_copy(8).start()
    start_own(wr_ring)
    attend_all((0, 1), 2, 2)
    kv_copy(7).wait_recv()
    kv_copy(8).wait_recv()
    attend_all((0, 1), 4, 2)
    attend_all((1, n_lead), 2, 1)
    kv_copy(5).wait_recv()
    kv_copy(6).wait_recv()
    kv_copy(9).start()
    attend_all((0, 1), 6, 1)
    attend_all((1, n_lead), 3, 1)
    kv_copy(9).wait_recv()
    attend_all((0, 1), 7, 1)
    finish(0)

    @pl.loop(1, n_lead)
    def _(i):
        @pl.loop(4, n_cp)
        def _(slot):
            attend(i, slot)

        finish(i)

    we_k = lambda k: functools.partial(we_ring, k)
    for k in range(n_tp - 1):
        we_swap(k).wait_recv()
    start_own(we_k(1))

    def late_chunk(i, first):
        @pl.loop(first, n_cp)
        def _(slot):
            attend(i, slot)

        finish(i)
        forward(ctx_copy, i - n_lead)

    late_chunk(n_lead, 2)
    pass_on(wr_ring)
    for k in range(2, n_tp):
        start_own(we_k(k))
    late_chunk(n_lead + 1, 0)
    pass_on(we_k(1))
    forward(ctx_copy, n_lead)
    pass_far(wr_ring)
    pass_on(we_k(2))
    forward(ctx_copy, n_lead + 1)
    for m in (2, 5, 6, 7):
        wr_ring(m).wait_recv()
    wr_copy().wait()

    @pl.loop(0, n_chunk)
    def _(i):
        ctx_copy(i, 2).wait_recv()
        ctx_copy(i, 3).wait_recv()
        sl = part_of(i, chunk)
        proj = jnp.dot(ct[0, sl, :], wr[0], preferred_element_type=jnp.float32)
        for t in range(1, n_tp):
            proj = proj + jnp.dot(ct[t, sl, :], wr[t], preferred_element_type=jnp.float32)
        out[sl, r_cols(tp)] = (out[sl, r_cols(tp)].astype(jnp.float32) + proj).astype(jnp.bfloat16)
        res_copy(i, 0).start()
        res_copy(i, 1).start()

    e_tile = 512
    n_e = e_cols // e_tile

    def project(j, first=False, last=False):
        ctx = jnp.concatenate([ct[t, :, part_of(j, piece)] for t in range(n_tp)], axis=1)

        @pl.loop(0, n_e)
        def _(n):
            sl = part_of(n, e_tile)
            w = we[j, :, :, sl].reshape(n_tp * piece, e_tile)
            add = jnp.dot(ctx, w, preferred_element_type=jnp.float32)
            if not first:
                add = acc_e[:, sl] + add
            if last:
                out[:, sl] = (out[:, sl].astype(jnp.float32) + add).astype(jnp.bfloat16)
            else:
                acc_e[:, sl] = add

    for j in range(n_cp):
        we_copy(j).wait()
    pass_on(we_k(3))
    project(own, first=True)
    forward(res_copy, 0)
    for k in range(1, n_tp):
        we_k(k)(2).wait_recv()
    project(at_x(0, 1))
    project(right)
    forward(res_copy, 1)
    pass_far(we_k(1))
    project(left)
    forward(res_copy, 2)
    pass_far(we_k(2))
    for k in range(1, n_tp):
        we_k(k)(5).wait_recv()
    project(at_x(-1, 1))
    for k in range(1, n_tp):
        we_k(k)(6).wait_recv()
    forward(res_copy, 3)
    pass_far(we_k(3))
    project(at_x(1, 1))
    project(far)
    for k in range(1, n_tp):
        we_k(k)(7).wait_recv()
    project(at_x(2, 1), last=True)

    @pl.loop(0, n_chunk)
    def _(i):
        res_copy(i, 2).wait_recv()
        res_copy(i, 3).wait_recv()

    for k in range(12):
        kv_copy(k).wait_send()
    for k in range(n_tp - 1):
        wr_swap(k).wait_send()
        we_swap(k).wait_send()
    for m in range(8):
        wr_ring(m).wait_send()
        for k in range(1, n_tp):
            we_ring(k, m).wait_send()

    @pl.loop(0, n_chunk)
    def _(i):
        for k in range(4):
            ctx_copy(i, k).wait_send()
            res_copy(i, k).wait_send()


def attention_block(mesh, pos, freq, gain, hidden, w_key, w_value, w_query, w_out):
    n_tp, n_cp = mesh.shape["tp"], mesh.shape["cp"]
    rows, width = hidden.shape
    kv_cols = w_key.shape[1]
    heads, kv_heads = w_query.shape[1] // HEAD, kv_cols // HEAD
    n_chunk = 4
    grp = heads // kv_heads * (rows // n_chunk)
    e_cols = width * E_FRACTION[0] // E_FRACTION[1]
    cols = (width - e_cols) // n_tp
    k_rows = w_out.shape[0]
    bf16, f32 = jnp.bfloat16, jnp.float32
    n_sem = 18 + 8 * n_tp + 8 * n_chunk
    cache = (rows, kv_heads, HEAD)
    return pl.pallas_call(
        functools.partial(block_kernel, n_tp, n_cp // 2),
        out_shape=[pltpu.VMEM(s, bf16) for s in ((rows, width), cache, cache)],
        in_specs=[vmem_spec()] * 3 + [any_spec()] * 5,
        out_specs=[vmem_spec()] * 3,
        scratch_shapes=[
            pltpu.VMEM((n_cp, rows + POS_ROWS, 2 * kv_cols), bf16),
            pltpu.VMEM((rows, width), bf16),
            pltpu.VMEM((rows, HEAD), f32),
            pltpu.VMEM((rows, HEAD), f32),
            pltpu.VMEM((N_Q, width, w_query.shape[1] // N_Q), bf16),
            pltpu.VMEM((n_tp, k_rows, cols), bf16),
            pltpu.VMEM((n_cp, n_tp, k_rows // n_cp, e_cols), bf16),
            pltpu.VMEM((n_tp, rows, k_rows), bf16),
            pltpu.VMEM((n_chunk, kv_heads, grp, HEAD), bf16),
            pltpu.VMEM((n_chunk, kv_heads, grp, HEAD), f32),
            pltpu.VMEM((n_chunk, kv_heads, grp, HEAD), f32),
            pltpu.VMEM((n_chunk, kv_heads, grp, HEAD), f32),
            pltpu.VMEM((rows, e_cols), f32),
            pltpu.VMEM((rows, HEAD), f32),
            pltpu.SemaphoreType.DMA((n_sem,)),
            pltpu.SemaphoreType.DMA((n_sem,)),
            pltpu.SemaphoreType.DMA((6 + N_Q + n_cp,)),
        ],
        compiler_params=pltpu.CompilerParams(collective_id=0, has_side_effects=True, vmem_limit_bytes=VMEM_LIMIT - 5 * 2**20),
        name="attention_block",
    )(pos, freq, gain, hidden, w_key, w_value, w_query, w_out)


def copy_kernel(src, k_src, v_src, dst, k_dst, v_dst, sem):
    n = 4
    tile = src.shape[0] // n
    rows = lambda i: pl.ds(i * tile, tile)
    copies = [pltpu.make_async_copy(src.at[rows(i)], dst.at[rows(i)], sem.at[i]) for i in range(n)]
    copies.append(pltpu.make_async_copy(k_src, k_dst, sem.at[n]))
    copies.append(pltpu.make_async_copy(v_src, v_dst, sem.at[n + 1]))
    for cpy in copies:
        cpy.start()
    for cpy in copies:
        cpy.wait()


def copy_out(*arrs):
    arrs = [pltpu.with_memory_space_constraint(a, pltpu.VMEM) for a in arrs]
    return pl.pallas_call(
        copy_kernel,
        in_specs=[vmem_spec()] * 3,
        out_specs=[any_spec()] * 3,
        out_shape=[jax.ShapeDtypeStruct(a.shape, a.dtype) for a in arrs],
        scratch_shapes=[pltpu.SemaphoreType.DMA((8,))],
        compiler_params=pltpu.CompilerParams(vmem_limit_bytes=4 * 2**20),
        name="copy_out",
    )(*arrs)


def solution(mesh):
    def local_block(hidden, tok_pos, norm_gain, w_query, w_key, w_value, w_out):
        results = attention_block(
            mesh, tok_pos.reshape(-1, HEAD), inv_freq_row(), norm_gain[None, :], hidden, w_key, w_value, w_query, w_out
        )
        return tuple(copy_out(*results))

    row_spec = P(("dp", "cp"), None)
    cache_spec = P(("dp", "cp"), "tp", None)
    return jax.shard_map(
        local_block,
        mesh=mesh,
        in_specs=(row_spec, P(("dp", "cp")), P(None), P(None, "tp"), P(None, "tp"), P(None, "tp"), P("tp", None)),
        out_specs=(row_spec, cache_spec, cache_spec),
        check_vma=False,
    )
```

```python
import functools

import jax
import jax.numpy as jnp
import numpy as np
from jax import lax
from jax.experimental import pallas as pl
from jax.experimental.pallas import tpu as pltpu
from jax.sharding import PartitionSpec as P

HEAD = 128
THETA = 1000000
EPS = 1e-5
NEG_BIG = -1e30
LOG2E = 1.4426950408889634
MESH = pl.DeviceIdType.MESH
VMEM_LIMIT = 64 * 2**20 - 64 * 2**10
POS_ROWS = 16
POS_BASE = 64
E_FRACTION = (3, 8)
N_Q = 4


def vmem_spec():
    return pl.BlockSpec(memory_space=pltpu.VMEM)


def any_spec():
    return pl.BlockSpec(memory_space=pl.ANY)


def inv_freq_row():
    freq = 1.0 / (np.float64(THETA) ** (np.arange(0, HEAD, 2) / HEAD))
    return jnp.asarray(np.concatenate([freq, freq])[None, :], jnp.float32)


def rope(head_f32, cos_full, sin_full):
    vals = head_f32.astype(jnp.bfloat16).astype(jnp.float32)
    return (vals * cos_full + pltpu.roll(vals, HEAD // 2, 1) * sin_full).astype(jnp.bfloat16)


def position_columns(pos_row):
    tiles = []
    for t in range(pos_row.shape[1] // HEAD):
        tile = jnp.broadcast_to(pos_row[:, t * HEAD : (t + 1) * HEAD], (HEAD, HEAD))
        tiles.append(jnp.transpose(tile))
    return jnp.concatenate(tiles, axis=0)


def block_kernel(
    n_tp, n_x, pos_hbm, freq_hbm, gain_hbm, hid_hbm, wk_hbm, wv_hbm, wq_hbm, wo_hbm, out, kc, vc,
    kv, r, cos, sin, wq, wr, we, ct, q, mx, ls, acc, acc_e, pos_q, pos_ref, freq_ref, gain_ref, ssem, rsem, lsem,
):
    rows, width = r.shape
    kv_cols = wk_hbm.shape[1]
    kv_heads = kv_cols // HEAD
    heads = wq_hbm.shape[1] // HEAD
    group = heads // kv_heads
    n_chunk, chunk = mx.shape[0], mx.shape[2] // group
    n_cp = 2 * n_x
    n_ring = 24 + 8 * n_tp
    half = rows // 2
    cols = wr.shape[2]
    e_cols = we.shape[3]
    piece = we.shape[2]
    q_cols = wq.shape[2]
    tp, cp = lax.axis_index("tp"), lax.axis_index("cp")
    x, core = cp // 2, cp % 2

    def at_x(dx, dc=0):
        return lax.rem(x + dx + n_x, n_x) * 2 + lax.rem(core + dc, 2)

    def at_y(dy):
        return lax.rem(tp + dy + n_tp, n_tp)

    x_right, x_left, partner = {"cp": at_x(1)}, {"cp": at_x(-1)}, {"cp": at_x(0, 1)}
    y_right, y_left, y_far = {"tp": at_y(1)}, {"tp": at_y(-1)}, {"tp": at_y(2)}

    def rc(src, dst, idx, dev):
        return pltpu.make_async_remote_copy(
            src_ref=src, dst_ref=dst, send_sem=ssem.at[idx], recv_sem=rsem.at[idx], device_id=dev, device_id_type=MESH
        )

    def lc(src, dst, idx):
        return pltpu.make_async_copy(src, dst, lsem.at[idx])

    def part_of(i, size, sub=None):
        if sub is None:
            return pl.ds(pl.multiple_of(i * size, size), size)
        return pl.ds(pl.multiple_of(i * size + sub * (size // 2), size // 2), size // 2)

    quarter = half // 2
    parts = (slice(0, quarter), slice(quarter, half), slice(half, rows))
    r_cols = lambda t: pl.ds(pl.multiple_of(e_cols + t * cols, HEAD), cols)
    hid_copy = lambda i: lc(hid_hbm.at[parts[i]], out.at[parts[i]], i)
    wk_copy = lambda: lc(wk_hbm, wq.at[N_Q - 2], 3)
    wv_copy = lambda: lc(wv_hbm, wq.at[N_Q - 1], 4)
    wq_copy = lambda c: lc(wq_hbm.at[:, part_of(c, q_cols)], wq.at[c], 5 + c)
    wr_copy = lambda: lc(wo_hbm.at[:, r_cols(tp)], wr.at[0], 5 + N_Q)
    we_copy = lambda j: lc(wo_hbm.at[part_of(j, piece), pl.ds(0, e_cols)], we.at[j, 0], 6 + N_Q + j)

    top, low = pl.ds(0, half), pl.ds(half, half + POS_ROWS)
    top_a, top_b = pl.ds(0, quarter), pl.ds(quarter, quarter)
    low_a, low_b = pl.ds(half, quarter), pl.ds(half + quarter, quarter + POS_ROWS)

    def kv_copy(k):
        src, dst, dev = (
            ((0, top_a), (2, top_a), x_right),
            ((0, top_a), (3, top_a), x_left),
            ((0, low), (3, low), x_left),
            ((0, low), (2, low), x_right),
            ((0,), (1,), partner),
            ((2, top_a), (6, top_a), x_right),
            ((3, top_b), (6, top_b), x_left),
            ((2,), (4,), partner),
            ((3,), (5,), partner),
            ((6, top_a), (7, top_a), partner),
            ((0, top_b), (2, top_b), x_right),
            ((0, top_b), (3, top_b), x_left),
            ((2, low_a), (6, low_a), x_right),
            ((3, low_b), (6, low_b), x_left),
            ((6, top_b), (7, top_b), partner),
            ((6, low_a), (7, low_a), partner),
            ((6, low_b), (7, low_b), partner),
        )[k]
        return rc(kv.at[src], kv.at[dst], k if k < 10 else n_ring - 7 + k - 10, dev)

    y_devs = (y_right, y_left, y_far)
    mine = part_of(cp, piece)

    def wr_swap(k):
        return rc(wo_hbm.at[mine, r_cols(at_y((1, -1, 2)[k]))], wr.at[1 + k, mine], 10 + k, y_devs[k])

    def we_swap(k):
        if k < 2:
            return rc(wo_hbm.at[mine, pl.ds(0, e_cols)], we.at[cp, 1 + k], 13 + k, y_devs[k])
        sub = part_of(k - 2, piece // 2)
        return rc(we.at[cp, k - 1, sub], we.at[cp, 3, sub], 15 if k == 2 else 16 + 8 * n_tp, y_devs[k - 2])

    own, right, left, far = cp, at_x(-1), at_x(1), at_x(2)
    ring = (
        (own, x_right, None), (own, x_left, None), (own, partner, None), (right, x_right, 0), (left, x_left, 1),
        (right, partner, None), (left, partner, None), (far, partner, None),
    )

    def wr_ring(m):
        src, dev, sub = ring[m]
        ref = wr.at[pl.ds(1, n_tp - 1), part_of(src, piece, sub)]
        return rc(ref, ref, 16 + m, dev)

    def we_ring(k, m):
        src, dev, sub = ring[m]
        ref = we.at[src, k] if sub is None else we.at[src, k, part_of(sub, piece // 2)]
        return rc(ref, ref, 16 + 8 * k + m, dev)

    def start_own(copy):
        for m in range(3):
            copy(m).start()

    def pass_on(copy):
        copy(0).wait_recv()
        copy(3).start()
        copy(5).start()
        copy(1).wait_recv()
        copy(4).start()
        copy(6).start()

    def pass_far(copy):
        copy(3).wait_recv()
        copy(4).wait_recv()
        copy(7).start()

    ctx_base = n_ring
    out_base = ctx_base + 4 * n_chunk

    def ctx_copy(i, k):
        src, dst, sub, dev = ((0, 1, None, y_right), (0, 2, None, y_left), (1, 3, 0, y_right), (2, 3, 1, y_left))[k]
        sl = part_of(i, chunk, sub)
        return rc(ct.at[src, sl], ct.at[dst, sl], ctx_base + 4 * i + k, dev)

    def res_copy(i, k):
        t, sub, dev = ((tp, None, y_right), (tp, None, y_left), (at_y(-1), 0, y_right), (at_y(1), 1, y_left))[k]
        ref = out.at[part_of(i, chunk, sub), r_cols(t)]
        return rc(ref, ref, out_base + 4 * i + k, dev)

    def forward(copy, i):
        copy(i, 0).wait_recv()
        copy(i, 2).start()
        copy(i, 1).wait_recv()
        copy(i, 3).start()

    barrier = pltpu.get_barrier_semaphore()
    peers = (x_right, x_left, partner) + y_devs
    for dev in peers:
        pl.semaphore_signal(barrier, inc=1, device_id=dev, device_id_type=MESH)
    small = [
        lc(a, b, 6 + N_Q + n_cp + t)
        for t, (a, b) in enumerate(((pos_hbm, pos_ref), (freq_hbm, freq_ref), (gain_hbm, gain_ref)))
    ]
    for cpy in small:
        cpy.start()
    hid_copy(0).start()
    wk_copy().start()
    wv_copy().start()

    for cpy in small:
        cpy.wait()
    pos = pos_ref[...]
    pos_row = jnp.concatenate([pos[t : t + 1] for t in range(pos.shape[0])], axis=1)
    pos_q[...] = position_columns(pos_row.astype(jnp.float32))
    angles = pos_q[...] * freq_ref[...]
    lane = lax.broadcasted_iota(jnp.int32, angles.shape, 1)
    sines = jnp.sin(angles)
    cos[...] = jnp.cos(angles)
    sin[...] = jnp.where(lane < HEAD // 2, -sines, sines)
    hi = jnp.broadcast_to((pos_row // POS_BASE).astype(jnp.float32), (POS_ROWS // 2, rows))
    lo = jnp.broadcast_to(lax.rem(pos_row, POS_BASE).astype(jnp.float32), (POS_ROWS // 2, rows))
    kv[0, rows:, :] = jnp.concatenate([hi, lo], axis=0).astype(jnp.bfloat16)

    for i, sl in enumerate(parts):
        hid_copy(i).wait()
        hid = out[sl, :].astype(jnp.float32)
        scaled = hid * lax.rsqrt(jnp.mean(hid * hid, axis=-1, keepdims=True) + EPS)
        r[sl, :] = (scaled * gain_ref[...]).astype(jnp.bfloat16)
        if i == 0:
            wk_copy().wait()
            wv_copy().wait()
            hid_copy(1).start()
            hid_copy(2).start()
            for c in range(N_Q - 2):
                wq_copy(c).start()
        k = jnp.dot(r[sl, :], wq[N_Q - 2], preferred_element_type=jnp.float32)
        v = jnp.dot(r[sl, :], wq[N_Q - 1], preferred_element_type=jnp.float32).astype(jnp.bfloat16)
        kv[0, sl, kv_cols:] = v
        rots = []
        for h in range(kv_heads):
            rots.append(rope(k[:, h * HEAD : (h + 1) * HEAD], cos[sl, :], sin[sl, :]))
            kv[0, sl, h * HEAD : (h + 1) * HEAD] = rots[h]
        if i == 0:
            pl.semaphore_wait(barrier, len(peers))
            kv_copy(0).start()
            kv_copy(1).start()
            for t in range(2):
                we_swap(t).start()
            for t in range(n_tp - 1):
                wr_swap(t).start()
        elif i == 1:
            kv_copy(10).start()
            kv_copy(11).start()
        else:
            kv_copy(2).start()
            kv_copy(3).start()
            kv_copy(4).start()
        kc[sl] = jnp.stack(rots, axis=1)
        vc[sl] = jnp.stack([v[:, h * HEAD : (h + 1) * HEAD] for h in range(kv_heads)], axis=1)
    for c in range(N_Q - 2, N_Q):
        wq_copy(c).start()
    wr_copy().start()
    for j in range(n_cp):
        we_copy(j).start()

    @pl.loop(0, N_Q)
    def _(c):
        wq_copy(c).wait()
        qc = jnp.dot(r[...], wq[c], preferred_element_type=jnp.float32)
        per = q_cols // HEAD
        for j in range(per):
            rot = rope(qc[:, j * HEAD : (j + 1) * HEAD], cos[...], sin[...])
            head = c * per + j
            kvh, g = head // group, lax.rem(head, group)
            for i in range(n_chunk):
                q[i, kvh, part_of(g, chunk), :] = rot[i * chunk : (i + 1) * chunk]

    mx[...] = jnp.full_like(mx, NEG_BIG)
    ls[...] = jnp.zeros_like(ls)
    acc[...] = jnp.zeros_like(acc)
    scale = HEAD**-0.5 * LOG2E

    def attend(i, slot, n_blk=1):
        pos_i = pos_q[part_of(i, chunk), :]
        n_l = n_blk * rows // HEAD
        biases = []
        for b in range(n_blk):
            hi = kv[slot + b, pl.ds(rows, POS_ROWS // 2), :].astype(jnp.float32)
            lo = kv[slot + b, pl.ds(rows + POS_ROWS // 2, POS_ROWS // 2), :].astype(jnp.float32)
            pos_k = (hi * POS_BASE + lo)[0:1, :]
            for t in range(rows // HEAD):
                biases.append(jnp.where(pos_k[:, t * HEAD : (t + 1) * HEAD] <= pos_i, 0.0, NEG_BIG))
        bias = jnp.concatenate(biases, axis=1)

        def block(b, first_col):
            return kv[slot + b, pl.ds(0, rows), first_col : first_col + HEAD]

        raw = [
            [
                lax.dot_general(
                    q[i, kvh], block(b, kvh * HEAD), (((1,), (1,)), ((), ())), preferred_element_type=jnp.float32
                )
                for b in range(n_blk)
            ]
            for kvh in range(kv_heads)
        ]
        for kvh in range(kv_heads):
            s = jnp.concatenate(raw[kvh], axis=1)
            s = (s.reshape(group, chunk, n_blk * rows) * scale + bias[None]).reshape(group * chunk, n_blk * rows)
            m_old = mx[i, kvh]
            m_new = jnp.maximum(m_old, jnp.max(s, axis=1, keepdims=True))
            alpha = jnp.exp2(m_old - m_new)
            p = jnp.exp2(s - jnp.concatenate([m_new] * n_l, axis=1))
            part = p[:, :HEAD]
            for t in range(1, n_l):
                part = part + p[:, t * HEAD : (t + 1) * HEAD]
            mx[i, kvh] = m_new
            ls[i, kvh] = ls[i, kvh] * alpha + part
            p = p.astype(jnp.bfloat16)
            pv = acc[i, kvh] * alpha
            for b in range(n_blk):
                pv = pv + jnp.dot(
                    p[:, b * rows : (b + 1) * rows], block(b, kv_cols + kvh * HEAD), preferred_element_type=jnp.float32
                )
            acc[i, kvh] = pv

    n_lead = n_chunk // 2

    def attend_each(chunks, slots):
        n_slot = slots[1] - slots[0]

        @pl.loop(0, (chunks[1] - chunks[0]) * n_slot)
        def _(t):
            attend(chunks[0] + t // n_slot, slots[0] + lax.rem(t, n_slot))

    def attend_rest(i, first):
        @pl.loop(0, (n_cp - first) // 2)
        def _(t):
            attend(i, first + 2 * t, 2)

    def finish(i):
        for kvh in range(kv_heads):
            total = jnp.sum(ls[i, kvh], axis=1, keepdims=True)
            ctx = (acc[i, kvh] / total).astype(jnp.bfloat16)
            for g in range(group):
                h = kvh * group + g
                ct[0, part_of(i, chunk), h * HEAD : (h + 1) * HEAD] = ctx[g * chunk : (g + 1) * chunk]
        ctx_copy(i, 0).start()
        ctx_copy(i, 1).start()

    kv_copy(0).wait_recv()
    kv_copy(5).start()
    attend_each((0, 1), (0, 1))
    kv_copy(11).wait_recv()
    kv_copy(6).start()
    kv_copy(10).wait_recv()
    kv_copy(1).wait_recv()
    attend_each((1, n_lead), (0, 1))
    for k in range(2):
        we_swap(k).wait_recv()
        we_swap(2 + k).start()
    kv_copy(4).wait_recv()
    attend_each((0, n_lead), (1, 2))
    kv_copy(3).wait_recv()
    kv_copy(12).start()
    kv_copy(7).start()
    kv_copy(2).wait_recv()
    kv_copy(13).start()
    kv_copy(8).start()
    attend_each((n_lead, n_lead + 1), (0, 2))
    attend_each((0, 1), (2, 4))
    kv_copy(5).wait_recv()
    kv_copy(9).start()
    kv_copy(6).wait_recv()
    kv_copy(14).start()
    kv_copy(7).wait_recv()
    kv_copy(8).wait_recv()
    attend_each((0, 1), (4, 5))
    for t in range(n_tp - 1):
        wr_swap(t).wait_recv()
    start_own(wr_ring)
    attend_each((0, 1), (5, 6))
    kv_copy(12).wait_recv()
    kv_copy(15).start()
    kv_copy(13).wait_recv()
    kv_copy(16).start()
    attend_each((0, 1), (6, 7))
    for k in (9, 14, 15, 16):
        kv_copy(k).wait_recv()
    attend_each((0, 1), (7, 8))
    finish(0)

    @pl.loop(1, n_lead)
    def _(i):
        attend_rest(i, 2)
        finish(i)

    we_k = lambda k: functools.partial(we_ring, k)
    for k in range(2, 4):
        we_swap(k).wait_recv()
    start_own(we_k(1))

    def late_chunk(i, first):
        attend_rest(i, first)
        finish(i)
        forward(ctx_copy, i - n_lead)

    late_chunk(n_lead, 2)
    pass_on(wr_ring)
    for k in range(2, n_tp):
        start_own(we_k(k))
    late_chunk(n_lead + 1, 0)
    pass_on(we_k(1))
    forward(ctx_copy, n_lead)
    pass_far(wr_ring)
    for m in (2, 5, 6, 7):
        wr_ring(m).wait_recv()
    wr_copy().wait()

    def project_own(i):
        ctx_copy(i, 2).wait_recv()
        ctx_copy(i, 3).wait_recv()
        sl = part_of(i, chunk)
        proj = jnp.dot(ct[0, sl, :], wr[0], preferred_element_type=jnp.float32)
        for t in range(1, n_tp):
            proj = proj + jnp.dot(ct[t, sl, :], wr[t], preferred_element_type=jnp.float32)
        out[sl, r_cols(tp)] = (out[sl, r_cols(tp)].astype(jnp.float32) + proj).astype(jnp.bfloat16)
        res_copy(i, 0).start()
        res_copy(i, 1).start()

    project_loop = lambda lo, hi: pl.loop(lo, hi)(project_own)
    project_loop(0, n_chunk - 3)
    forward(ctx_copy, n_lead + 1)
    project_loop(n_chunk - 3, n_chunk - 2)
    pass_on(we_k(2))
    project_loop(n_chunk - 2, n_chunk)

    e_tile = 512
    n_e = e_cols // e_tile

    def project(j, first=False, last=False):
        ctx = jnp.concatenate([ct[t, :, part_of(j, piece)] for t in range(n_tp)], axis=1)

        @pl.loop(0, n_e)
        def _(n):
            sl = part_of(n, e_tile)
            w = we[j, :, :, sl].reshape(n_tp * piece, e_tile)
            add = jnp.dot(ctx, w, preferred_element_type=jnp.float32)
            if not first:
                add = acc_e[:, sl] + add
            if last:
                out[:, sl] = (out[:, sl].astype(jnp.float32) + add).astype(jnp.bfloat16)
            else:
                acc_e[:, sl] = add

    for j in range(n_cp):
        we_copy(j).wait()
    pass_on(we_k(3))
    project(own, first=True)
    forward(res_copy, 0)
    for k in range(1, n_tp):
        we_k(k)(2).wait_recv()
    project(at_x(0, 1))
    project(right)
    forward(res_copy, 1)
    pass_far(we_k(1))
    project(left)
    forward(res_copy, 2)
    pass_far(we_k(2))
    for k in range(1, n_tp):
        we_k(k)(5).wait_recv()
    project(at_x(-1, 1))
    for k in range(1, n_tp):
        we_k(k)(6).wait_recv()
    forward(res_copy, 3)
    pass_far(we_k(3))
    project(at_x(1, 1))
    project(far)
    for k in range(1, n_tp):
        we_k(k)(7).wait_recv()
    project(at_x(2, 1), last=True)

    @pl.loop(0, n_chunk)
    def _(i):
        res_copy(i, 2).wait_recv()
        res_copy(i, 3).wait_recv()

    for k in range(17):
        kv_copy(k).wait_send()
    for k in range(n_tp - 1):
        wr_swap(k).wait_send()
    for k in range(4):
        we_swap(k).wait_send()
    for m in range(8):
        wr_ring(m).wait_send()
        for k in range(1, n_tp):
            we_ring(k, m).wait_send()

    @pl.loop(0, n_chunk)
    def _(i):
        for k in range(4):
            ctx_copy(i, k).wait_send()
            res_copy(i, k).wait_send()


def attention_block(mesh, pos, freq, gain, hidden, w_key, w_value, w_query, w_out):
    n_tp, n_cp = mesh.shape["tp"], mesh.shape["cp"]
    rows, width = hidden.shape
    kv_cols = w_key.shape[1]
    heads, kv_heads = w_query.shape[1] // HEAD, kv_cols // HEAD
    n_chunk = 4
    grp = heads // kv_heads * (rows // n_chunk)
    e_cols = width * E_FRACTION[0] // E_FRACTION[1]
    cols = (width - e_cols) // n_tp
    k_rows = w_out.shape[0]
    bf16, f32 = jnp.bfloat16, jnp.float32
    n_sem = 24 + 8 * n_tp + 8 * n_chunk
    cache = (rows, kv_heads, HEAD)
    return pl.pallas_call(
        functools.partial(block_kernel, n_tp, n_cp // 2),
        out_shape=[pltpu.VMEM(s, bf16) for s in ((rows, width), cache, cache)],
        in_specs=[any_spec()] * 8,
        out_specs=[vmem_spec()] * 3,
        scratch_shapes=[
            pltpu.VMEM((n_cp, rows + POS_ROWS, 2 * kv_cols), bf16),
            pltpu.VMEM((rows, width), bf16),
            pltpu.VMEM((rows, HEAD), f32),
            pltpu.VMEM((rows, HEAD), f32),
            pltpu.VMEM((N_Q, width, w_query.shape[1] // N_Q), bf16),
            pltpu.VMEM((n_tp, k_rows, cols), bf16),
            pltpu.VMEM((n_cp, n_tp, k_rows // n_cp, e_cols), bf16),
            pltpu.VMEM((n_tp, rows, k_rows), bf16),
            pltpu.VMEM((n_chunk, kv_heads, grp, HEAD), bf16),
            pltpu.VMEM((n_chunk, kv_heads, grp, HEAD), f32),
            pltpu.VMEM((n_chunk, kv_heads, grp, HEAD), f32),
            pltpu.VMEM((n_chunk, kv_heads, grp, HEAD), f32),
            pltpu.VMEM((rows, e_cols), f32),
            pltpu.VMEM((rows, HEAD), f32),
            pltpu.VMEM(pos.shape, pos.dtype),
            pltpu.VMEM(freq.shape, f32),
            pltpu.VMEM(gain.shape, f32),
            pltpu.SemaphoreType.DMA((n_sem,)),
            pltpu.SemaphoreType.DMA((n_sem,)),
            pltpu.SemaphoreType.DMA((9 + N_Q + n_cp,)),
        ],
        compiler_params=pltpu.CompilerParams(collective_id=0, has_side_effects=True, vmem_limit_bytes=VMEM_LIMIT - 5 * 2**20),
        name="attention_block",
    )(pos, freq, gain, hidden, w_key, w_value, w_query, w_out)


def copy_kernel(src, k_src, v_src, dst, k_dst, v_dst, sem):
    n = 4
    tile = src.shape[0] // n
    rows = lambda i: pl.ds(i * tile, tile)
    copies = [pltpu.make_async_copy(src.at[rows(i)], dst.at[rows(i)], sem.at[i]) for i in range(n)]
    copies.append(pltpu.make_async_copy(k_src, k_dst, sem.at[n]))
    copies.append(pltpu.make_async_copy(v_src, v_dst, sem.at[n + 1]))
    for cpy in copies:
        cpy.start()
    for cpy in copies:
        cpy.wait()


def copy_out(*arrs):
    arrs = [pltpu.with_memory_space_constraint(a, pltpu.VMEM) for a in arrs]
    return pl.pallas_call(
        copy_kernel,
        in_specs=[vmem_spec()] * 3,
        out_specs=[any_spec()] * 3,
        out_shape=[jax.ShapeDtypeStruct(a.shape, a.dtype) for a in arrs],
        scratch_shapes=[pltpu.SemaphoreType.DMA((8,))],
        compiler_params=pltpu.CompilerParams(vmem_limit_bytes=4 * 2**20),
        name="copy_out",
    )(*arrs)


def solution(mesh):
    def local_block(hidden, tok_pos, norm_gain, w_query, w_key, w_value, w_out):
        results = attention_block(
            mesh, tok_pos.reshape(-1, HEAD), inv_freq_row(), norm_gain[None, :], hidden, w_key, w_value, w_query, w_out
        )
        return tuple(copy_out(*results))

    row_spec = P(("dp", "cp"), None)
    cache_spec = P(("dp", "cp"), "tp", None)
    return jax.shard_map(
        local_block,
        mesh=mesh,
        in_specs=(row_spec, P(("dp", "cp")), P(None), P(None, "tp"), P(None, "tp"), P(None, "tp"), P("tp", None)),
        out_specs=(row_spec, cache_spec, cache_spec),
        check_vma=False,
    )
```

```python
import functools

import jax
import jax.numpy as jnp
import numpy as np
from jax import lax
from jax.experimental import pallas as pl
from jax.experimental.pallas import tpu as pltpu
from jax.sharding import PartitionSpec as P

HEAD = 128
THETA = 1000000
EPS = 1e-5
NEG_BIG = -1e30
LOG2E = 1.4426950408889634
MESH = pl.DeviceIdType.MESH
VMEM_LIMIT = 64 * 2**20 - 64 * 2**10
POS_ROWS = 16
POS_BASE = 64
E_FRACTION = (3, 8)
N_Q = 4


def vmem_spec():
    return pl.BlockSpec(memory_space=pltpu.VMEM)


def any_spec():
    return pl.BlockSpec(memory_space=pl.ANY)


def inv_freq_row():
    freq = 1.0 / (np.float64(THETA) ** (np.arange(0, HEAD, 2) / HEAD))
    return jnp.asarray(np.concatenate([freq, freq])[None, :], jnp.float32)


def rope(head_f32, cos_full, sin_full):
    vals = head_f32.astype(jnp.bfloat16).astype(jnp.float32)
    return (vals * cos_full + pltpu.roll(vals, HEAD // 2, 1) * sin_full).astype(jnp.bfloat16)


def position_columns(pos_row):
    tiles = []
    for t in range(pos_row.shape[1] // HEAD):
        tile = jnp.broadcast_to(pos_row[:, t * HEAD : (t + 1) * HEAD], (HEAD, HEAD))
        tiles.append(jnp.transpose(tile))
    return jnp.concatenate(tiles, axis=0)


def block_kernel(
    n_tp, n_x, pos_hbm, freq_hbm, gain_hbm, hid_hbm, wk_hbm, wv_hbm, wq_hbm, wo_hbm, out, kc, vc,
    kv, r, cos, sin, wq, wr, we, ct, q, mx, ls, acc, acc_e, pos_q, pos_ref, freq_ref, gain_ref, ssem, rsem, lsem,
):
    rows, width = r.shape
    kv_cols = wk_hbm.shape[1]
    kv_heads = kv_cols // HEAD
    heads = wq_hbm.shape[1] // HEAD
    group = heads // kv_heads
    n_chunk, chunk = mx.shape[0], mx.shape[2] // group
    n_cp = 2 * n_x
    n_hop = 9
    n_ring = 26 + n_hop * n_tp
    half = rows // 2
    cols = wr.shape[2]
    e_cols = we.shape[3]
    piece = we.shape[2]
    q_cols = wq.shape[2]
    tp, cp = lax.axis_index("tp"), lax.axis_index("cp")
    x, core = cp // 2, cp % 2

    def at_x(dx, dc=0):
        return lax.rem(x + dx + n_x, n_x) * 2 + lax.rem(core + dc, 2)

    def at_y(dy):
        return lax.rem(tp + dy + n_tp, n_tp)

    x_right, x_left, partner = {"cp": at_x(1)}, {"cp": at_x(-1)}, {"cp": at_x(0, 1)}
    y_right, y_left, y_far = {"tp": at_y(1)}, {"tp": at_y(-1)}, {"tp": at_y(2)}

    def rc(src, dst, idx, dev, send=None):
        return pltpu.make_async_remote_copy(
            src_ref=src,
            dst_ref=dst,
            send_sem=ssem.at[idx if send is None else send],
            recv_sem=rsem.at[idx],
            device_id=dev,
            device_id_type=MESH,
        )

    def lc(src, dst, idx):
        return pltpu.make_async_copy(src, dst, lsem.at[idx])

    def part_of(i, size, sub=None):
        if sub is None:
            return pl.ds(pl.multiple_of(i * size, size), size)
        return pl.ds(pl.multiple_of(i * size + sub * (size // 2), size // 2), size // 2)

    quarter = half // 2
    parts = (slice(0, quarter), slice(quarter, half), slice(half, rows))
    r_cols = lambda t: pl.ds(pl.multiple_of(e_cols + t * cols, HEAD), cols)
    hid_copy = lambda i: lc(hid_hbm.at[parts[i]], out.at[parts[i]], i)
    wk_copy = lambda: lc(wk_hbm, wq.at[N_Q - 2], 3)
    wv_copy = lambda: lc(wv_hbm, wq.at[N_Q - 1], 4)
    wq_copy = lambda c: lc(wq_hbm.at[:, part_of(c, q_cols)], wq.at[c], 5 + c)
    wr_copy = lambda: lc(wo_hbm.at[:, r_cols(tp)], wr.at[0], 5 + N_Q)
    we_copy = lambda j: lc(wo_hbm.at[part_of(j, piece), pl.ds(0, e_cols)], we.at[j, 0], 6 + N_Q + j)

    top, low = pl.ds(0, half), pl.ds(half, half + POS_ROWS)
    top_a, top_b = pl.ds(0, quarter), pl.ds(quarter, quarter)
    k_cols, v_cols = pl.ds(0, kv_cols), pl.ds(kv_cols, kv_cols)
    low_a, low_b = pl.ds(half, quarter), pl.ds(half + quarter, quarter + POS_ROWS)

    def kv_copy(k):
        src, dst, dev = (
            ((0, top_a, v_cols), (2, top_a, v_cols), x_right),
            ((0, top_a, v_cols), (3, top_a, v_cols), x_left),
            ((0, low), (3, low), x_left),
            ((0, low), (2, low), x_right),
            ((0,), (1,), partner),
            ((2, top_a), (6, top_a), x_right),
            ((3, top_b), (6, top_b), x_left),
            ((2,), (4,), partner),
            ((3,), (5,), partner),
            ((6, top_a), (7, top_a), partner),
            ((0, top_b), (2, top_b), x_right),
            ((0, top_b), (3, top_b), x_left),
            ((2, low_a), (6, low_a), x_right),
            ((3, low_b), (6, low_b), x_left),
            ((6, top_b), (7, top_b), partner),
            ((6, low_a), (7, low_a), partner),
            ((6, low_b), (7, low_b), partner),
            ((0, top_a, k_cols), (2, top_a, k_cols), x_right),
            ((0, top_a, k_cols), (3, top_a, k_cols), x_left),
        )[k]
        return rc(kv.at[src], kv.at[dst], k if k < 10 else n_ring - 9 + k - 10, dev)

    y_devs = (y_right, y_left, y_far)
    mine = part_of(cp, piece)

    def wr_swap(k):
        return rc(wo_hbm.at[mine, r_cols(at_y((1, -1, 2)[k]))], wr.at[1 + k, mine], 10 + k, y_devs[k])

    def we_swap(k):
        if k < 2:
            return rc(wo_hbm.at[mine, pl.ds(0, e_cols)], we.at[cp, 1 + k], 13 + k, y_devs[k])
        sub = part_of(k - 2, piece // 2)
        return rc(we.at[cp, k - 1, sub], we.at[cp, 3, sub], 15 if k == 2 else 16 + n_hop * n_tp, y_devs[k - 2])

    own, right, left, far = cp, at_x(-1), at_x(1), at_x(2)
    ring = (
        (own, x_right, None), (own, x_left, None), (own, partner, None), (right, x_right, 0), (left, x_left, 1),
        (right, partner, None), (left, partner, None), (far, partner, 0), (far, partner, 1),
    )

    def wr_ring(m):
        src, dev, sub = ring[m]
        ref = wr.at[pl.ds(1, n_tp - 1), part_of(src, piece, sub)]
        return rc(ref, ref, 16 + m, dev)

    def we_ring(k, m):
        src, dev, sub = ring[m]
        ref = we.at[src, k] if sub is None else we.at[src, k, part_of(sub, piece // 2)]
        return rc(ref, ref, 16 + n_hop * k + m, dev)

    def start_own(copy):
        for m in range(3):
            copy(m).start()

    def pass_on(copy):
        copy(0).wait_recv()
        copy(3).start()
        copy(5).start()
        copy(1).wait_recv()
        copy(4).start()
        copy(6).start()

    def pass_far(copy):
        copy(3).wait_recv()
        copy(7).start()
        copy(4).wait_recv()
        copy(8).start()

    ctx_base = n_ring
    out_base = ctx_base + 4 * n_chunk

    def ctx_copy(i, k):
        src, dst, sub, dev = ((0, 1, None, y_right), (0, 2, None, y_left), (1, 3, 0, y_right), (2, 3, 1, y_left))[k]
        sl = part_of(i, chunk, sub)
        return rc(ct.at[src, sl], ct.at[dst, sl], ctx_base + 4 * i + k, dev, 4 * i + k)

    def res_copy(i, k):
        t, sub, dev = ((tp, None, y_right), (tp, None, y_left), (at_y(-1), 0, y_right), (at_y(1), 1, y_left))[k]
        ref = out.at[part_of(i, chunk, sub), r_cols(t)]
        return rc(ref, ref, out_base + 4 * i + k, dev, 4 * i + k)

    def forward(copy, i):
        copy(i, 0).wait_recv()
        copy(i, 2).start()
        copy(i, 1).wait_recv()
        copy(i, 3).start()

    def forward_res(i):
        ctx_copy(i, 2).wait_send()
        ctx_copy(i, 3).wait_send()
        forward(res_copy, i)

    barrier = pltpu.get_barrier_semaphore()
    peers = (x_right, x_left, partner) + y_devs
    for dev in peers:
        pl.semaphore_signal(barrier, inc=1, device_id=dev, device_id_type=MESH)
    small = [
        lc(a, b, 6 + N_Q + n_cp + t)
        for t, (a, b) in enumerate(((gain_hbm, gain_ref), (pos_hbm, pos_ref), (freq_hbm, freq_ref)))
    ]
    small[0].start()
    hid_copy(0).start()
    wv_copy().start()
    wk_copy().start()
    small[1].start()
    small[2].start()
    hid_copy(1).start()
    hid_copy(2).start()
    for c in range(N_Q - 2):
        wq_copy(c).start()

    def normalise(sl):
        hid = out[sl, :].astype(jnp.float32)
        scaled = hid * lax.rsqrt(jnp.mean(hid * hid, axis=-1, keepdims=True) + EPS)
        r[sl, :] = (scaled * gain_ref[...]).astype(jnp.bfloat16)

    def product(sl, w):
        return jnp.dot(r[sl, :], wq[w], preferred_element_type=jnp.float32)

    def put_v(sl, v):
        v = v.astype(jnp.bfloat16)
        kv[0, sl, kv_cols:] = v
        vc[sl] = jnp.stack([v[:, h * HEAD : (h + 1) * HEAD] for h in range(kv_heads)], axis=1)

    def put_k(sl, k):
        rots = []
        for h in range(kv_heads):
            rots.append(rope(k[:, h * HEAD : (h + 1) * HEAD], cos[sl, :], sin[sl, :]))
            kv[0, sl, h * HEAD : (h + 1) * HEAD] = rots[h]
        kc[sl] = jnp.stack(rots, axis=1)

    def project_kv(sl):
        k, v = product(sl, N_Q - 2), product(sl, N_Q - 1)
        put_v(sl, v)
        put_k(sl, k)

    small[0].wait()
    hid_copy(0).wait()
    normalise(parts[0])
    wv_copy().wait()
    put_v(parts[0], product(parts[0], N_Q - 1))
    pl.semaphore_wait(barrier, len(peers))
    kv_copy(0).start()
    kv_copy(1).start()
    for t in range(2):
        we_swap(t).start()
    for t in range(n_tp - 1):
        wr_swap(t).start()

    small[1].wait()
    small[2].wait()
    pos = pos_ref[...]
    pos_row = jnp.concatenate([pos[t : t + 1] for t in range(pos.shape[0])], axis=1)
    pos_q[...] = position_columns(pos_row.astype(jnp.float32))
    angles = pos_q[...] * freq_ref[...]
    lane = lax.broadcasted_iota(jnp.int32, angles.shape, 1)
    sines = jnp.sin(angles)
    cos[...] = jnp.cos(angles)
    sin[...] = jnp.where(lane < HEAD // 2, -sines, sines)
    hi = jnp.broadcast_to((pos_row // POS_BASE).astype(jnp.float32), (POS_ROWS // 2, rows))
    lo = jnp.broadcast_to(lax.rem(pos_row, POS_BASE).astype(jnp.float32), (POS_ROWS // 2, rows))
    kv[0, rows:, :] = jnp.concatenate([hi, lo], axis=0).astype(jnp.bfloat16)

    wk_copy().wait()
    put_k(parts[0], product(parts[0], N_Q - 2))
    kv_copy(17).start()
    kv_copy(18).start()
    hid_copy(1).wait()
    normalise(parts[1])
    project_kv(parts[1])
    kv_copy(10).start()
    kv_copy(11).start()
    hid_copy(2).wait()
    normalise(parts[2])
    project_kv(parts[2])
    kv_copy(2).start()
    kv_copy(3).start()
    kv_copy(4).start()
    for c in range(N_Q - 2, N_Q):
        wq_copy(c).start()
    wr_copy().start()
    for j in range(n_cp):
        we_copy(j).start()

    @pl.loop(0, N_Q)
    def _(c):
        wq_copy(c).wait()
        qc = jnp.dot(r[...], wq[c], preferred_element_type=jnp.float32)
        per = q_cols // HEAD
        for j in range(per):
            rot = rope(qc[:, j * HEAD : (j + 1) * HEAD], cos[...], sin[...])
            head = c * per + j
            kvh, g = head // group, lax.rem(head, group)
            for i in range(n_chunk):
                q[i, kvh, part_of(g, chunk), :] = rot[i * chunk : (i + 1) * chunk]

    mx[...] = jnp.full_like(mx, NEG_BIG)
    ls[...] = jnp.zeros_like(ls)
    acc[...] = jnp.zeros_like(acc)
    scale = HEAD**-0.5 * LOG2E

    def attend(i, slot, n_blk=1):
        pos_i = pos_q[part_of(i, chunk), :]
        n_l = n_blk * rows // HEAD
        biases = []
        for b in range(n_blk):
            hi = kv[slot + b, pl.ds(rows, POS_ROWS // 2), :].astype(jnp.float32)
            lo = kv[slot + b, pl.ds(rows + POS_ROWS // 2, POS_ROWS // 2), :].astype(jnp.float32)
            pos_k = (hi * POS_BASE + lo)[0:1, :]
            for t in range(rows // HEAD):
                biases.append(jnp.where(pos_k[:, t * HEAD : (t + 1) * HEAD] <= pos_i, 0.0, NEG_BIG))
        bias = jnp.concatenate(biases, axis=1)

        def block(b, first_col):
            return kv[slot + b, pl.ds(0, rows), first_col : first_col + HEAD]

        raw = [
            [
                lax.dot_general(
                    q[i, kvh], block(b, kvh * HEAD), (((1,), (1,)), ((), ())), preferred_element_type=jnp.float32
                )
                for b in range(n_blk)
            ]
            for kvh in range(kv_heads)
        ]
        for kvh in range(kv_heads):
            s = jnp.concatenate(raw[kvh], axis=1)
            s = (s.reshape(group, chunk, n_blk * rows) * scale + bias[None]).reshape(group * chunk, n_blk * rows)
            m_old = mx[i, kvh]
            m_new = jnp.maximum(m_old, jnp.max(s, axis=1, keepdims=True))
            alpha = jnp.exp2(m_old - m_new)
            p = jnp.exp2(s - jnp.concatenate([m_new] * n_l, axis=1))
            part = p[:, :HEAD]
            for t in range(1, n_l):
                part = part + p[:, t * HEAD : (t + 1) * HEAD]
            mx[i, kvh] = m_new
            ls[i, kvh] = ls[i, kvh] * alpha + part
            p = p.astype(jnp.bfloat16)
            pv = acc[i, kvh] * alpha
            for b in range(n_blk):
                pv = pv + jnp.dot(
                    p[:, b * rows : (b + 1) * rows], block(b, kv_cols + kvh * HEAD), preferred_element_type=jnp.float32
                )
            acc[i, kvh] = pv

    n_lead = n_chunk // 2

    def attend_each(chunks, slots):
        n_slot = slots[1] - slots[0]

        @pl.loop(0, (chunks[1] - chunks[0]) * n_slot)
        def _(t):
            attend(chunks[0] + t // n_slot, slots[0] + lax.rem(t, n_slot))

    def attend_some(i, first, last):
        @pl.loop(0, (last - first) // 2)
        def _(t):
            attend(i, first + 2 * t, 2)

    def finish(i):
        for kvh in range(kv_heads):
            total = jnp.sum(ls[i, kvh], axis=1, keepdims=True)
            ctx = (acc[i, kvh] / total).astype(jnp.bfloat16)
            for g in range(group):
                h = kvh * group + g
                ct[0, part_of(i, chunk), h * HEAD : (h + 1) * HEAD] = ctx[g * chunk : (g + 1) * chunk]
        ctx_copy(i, 0).start()
        ctx_copy(i, 1).start()

    kv_copy(0).wait_recv()
    kv_copy(17).wait_recv()
    kv_copy(5).start()
    attend_each((0, 1), (0, 1))
    kv_copy(11).wait_recv()
    kv_copy(6).start()
    kv_copy(10).wait_recv()
    kv_copy(1).wait_recv()
    kv_copy(18).wait_recv()
    attend_each((1, n_lead), (0, 1))
    for k in range(2):
        we_swap(k).wait_recv()
        we_swap(2 + k).start()
    kv_copy(4).wait_recv()
    attend_each((0, 1), (1, 2))
    kv_copy(3).wait_recv()
    kv_copy(12).start()
    kv_copy(7).start()
    kv_copy(2).wait_recv()
    kv_copy(13).start()
    kv_copy(8).start()
    attend_each((1, n_lead), (1, 2))
    attend_each((0, 1), (2, 4))
    kv_copy(5).wait_recv()
    kv_copy(9).start()
    kv_copy(6).wait_recv()
    kv_copy(14).start()
    kv_copy(7).wait_recv()
    kv_copy(8).wait_recv()
    attend_each((0, 1), (4, 5))
    for t in range(n_tp - 1):
        wr_swap(t).wait_recv()
    start_own(wr_ring)
    attend_each((0, 1), (5, 6))
    kv_copy(12).wait_recv()
    kv_copy(15).start()
    kv_copy(13).wait_recv()
    kv_copy(16).start()
    attend_each((0, 1), (6, 7))
    for k in (9, 14, 15, 16):
        kv_copy(k).wait_recv()
    attend_each((0, 1), (7, 8))
    for k in range(19):
        kv_copy(k).wait_send()
    for k in range(n_tp - 1):
        wr_swap(k).wait_send()
        we_swap(k).wait_send()
    finish(0)

    @pl.loop(1, n_lead)
    def _(i):
        attend_some(i, 2, n_cp)
        finish(i)

    we_k = lambda k: functools.partial(we_ring, k)
    for k in range(2, 4):
        we_swap(k).wait_recv()
    start_own(we_k(1))

    def late_chunk(i):
        attend_some(i, 0, n_cp // 2)
        forward(ctx_copy, i - n_lead)
        attend_some(i, n_cp // 2, n_cp)
        finish(i)

    late_chunk(n_lead)
    pass_on(wr_ring)
    for k in range(2, n_tp):
        start_own(we_k(k))
    late_chunk(n_lead + 1)
    pass_on(we_k(1))
    forward(ctx_copy, n_lead)
    pass_far(wr_ring)
    for m in (2, 5, 6, 7, 8):
        wr_ring(m).wait_recv()
    wr_copy().wait()

    def project_own(i):
        ctx_copy(i, 2).wait_recv()
        ctx_copy(i, 3).wait_recv()
        sl = part_of(i, chunk)
        proj = jnp.dot(ct[0, sl, :], wr[0], preferred_element_type=jnp.float32)
        for t in range(1, n_tp):
            proj = proj + jnp.dot(ct[t, sl, :], wr[t], preferred_element_type=jnp.float32)
        out[sl, r_cols(tp)] = (out[sl, r_cols(tp)].astype(jnp.float32) + proj).astype(jnp.bfloat16)
        for k in range(2):
            ctx_copy(i, k).wait_send()
            res_copy(i, k).start()

    project_loop = lambda lo, hi: pl.loop(lo, hi)(project_own)
    project_loop(0, n_chunk - 3)
    forward(ctx_copy, n_lead + 1)
    project_loop(n_chunk - 3, n_chunk - 2)
    pass_on(we_k(2))
    project_loop(n_chunk - 2, n_chunk)

    e_tile = 512
    n_e = e_cols // e_tile

    def project(j, first=False, last=False):
        ctx = jnp.concatenate([ct[t, :, part_of(j, piece)] for t in range(n_tp)], axis=1)

        @pl.loop(0, n_e)
        def _(n):
            sl = part_of(n, e_tile)
            w = we[j, :, :, sl].reshape(n_tp * piece, e_tile)
            add = jnp.dot(ctx, w, preferred_element_type=jnp.float32)
            if not first:
                add = acc_e[:, sl] + add
            if last:
                out[:, sl] = (out[:, sl].astype(jnp.float32) + add).astype(jnp.bfloat16)
            else:
                acc_e[:, sl] = add

    for j in range(n_cp):
        we_copy(j).wait()
    pass_on(we_k(3))
    project(own, first=True)
    forward_res(0)
    for k in range(1, n_tp):
        we_k(k)(2).wait_recv()
    project(at_x(0, 1))
    project(right)
    forward_res(1)
    pass_far(we_k(1))
    project(left)
    forward_res(2)
    pass_far(we_k(2))
    for k in range(1, n_tp):
        we_k(k)(5).wait_recv()
    project(at_x(-1, 1))
    for k in range(1, n_tp):
        we_k(k)(6).wait_recv()
    forward_res(3)
    project(at_x(1, 1))
    pass_far(we_k(3))
    project(far)
    for k in range(1, n_tp):
        we_k(k)(7).wait_recv()
        we_k(k)(8).wait_recv()
    project(at_x(2, 1), last=True)

    @pl.loop(0, n_chunk)
    def _(i):
        res_copy(i, 2).wait_recv()
        res_copy(i, 3).wait_recv()

    we_swap(3).wait_send()
    for m in range(n_hop):
        wr_ring(m).wait_send()
        for k in range(1, n_tp):
            we_ring(k, m).wait_send()

    @pl.loop(0, n_chunk)
    def _(i):
        for k in range(4):
            res_copy(i, k).wait_send()


def attention_block(mesh, pos, freq, gain, hidden, w_key, w_value, w_query, w_out):
    n_tp, n_cp = mesh.shape["tp"], mesh.shape["cp"]
    rows, width = hidden.shape
    kv_cols = w_key.shape[1]
    heads, kv_heads = w_query.shape[1] // HEAD, kv_cols // HEAD
    n_chunk = 4
    grp = heads // kv_heads * (rows // n_chunk)
    e_cols = width * E_FRACTION[0] // E_FRACTION[1]
    cols = (width - e_cols) // n_tp
    k_rows = w_out.shape[0]
    bf16, f32 = jnp.bfloat16, jnp.float32
    n_sem = 26 + 9 * n_tp + 8 * n_chunk
    cache = (rows, kv_heads, HEAD)
    return pl.pallas_call(
        functools.partial(block_kernel, n_tp, n_cp // 2),
        out_shape=[pltpu.VMEM(s, bf16) for s in ((rows, width), cache, cache)],
        in_specs=[any_spec()] * 8,
        out_specs=[vmem_spec()] * 3,
        scratch_shapes=[
            pltpu.VMEM((n_cp, rows + POS_ROWS, 2 * kv_cols), bf16),
            pltpu.VMEM((rows, width), bf16),
            pltpu.VMEM((rows, HEAD), f32),
            pltpu.VMEM((rows, HEAD), f32),
            pltpu.VMEM((N_Q, width, w_query.shape[1] // N_Q), bf16),
            pltpu.VMEM((n_tp, k_rows, cols), bf16),
            pltpu.VMEM((n_cp, n_tp, k_rows // n_cp, e_cols), bf16),
            pltpu.VMEM((n_tp, rows, k_rows), bf16),
            pltpu.VMEM((n_chunk, kv_heads, grp, HEAD), bf16),
            pltpu.VMEM((n_chunk, kv_heads, grp, HEAD), f32),
            pltpu.VMEM((n_chunk, kv_heads, grp, HEAD), f32),
            pltpu.VMEM((n_chunk, kv_heads, grp, HEAD), f32),
            pltpu.VMEM((rows, e_cols), f32),
            pltpu.VMEM((rows, HEAD), f32),
            pltpu.VMEM(pos.shape, pos.dtype),
            pltpu.VMEM(freq.shape, f32),
            pltpu.VMEM(gain.shape, f32),
            pltpu.SemaphoreType.DMA((n_sem - 8 * n_chunk,)),
            pltpu.SemaphoreType.DMA((n_sem,)),
            pltpu.SemaphoreType.DMA((9 + N_Q + n_cp,)),
        ],
        compiler_params=pltpu.CompilerParams(collective_id=0, has_side_effects=True, vmem_limit_bytes=VMEM_LIMIT - 5 * 2**20),
        name="attention_block",
    )(pos, freq, gain, hidden, w_key, w_value, w_query, w_out)


def copy_kernel(src, k_src, v_src, dst, k_dst, v_dst, sem):
    n = 4
    tile = src.shape[0] // n
    rows = lambda i: pl.ds(i * tile, tile)
    copies = [pltpu.make_async_copy(src.at[rows(i)], dst.at[rows(i)], sem.at[i]) for i in range(n)]
    copies.append(pltpu.make_async_copy(k_src, k_dst, sem.at[n]))
    copies.append(pltpu.make_async_copy(v_src, v_dst, sem.at[n + 1]))
    for cpy in copies:
        cpy.start()
    for cpy in copies:
        cpy.wait()


def copy_out(*arrs):
    arrs = [pltpu.with_memory_space_constraint(a, pltpu.VMEM) for a in arrs]
    return pl.pallas_call(
        copy_kernel,
        in_specs=[vmem_spec()] * 3,
        out_specs=[any_spec()] * 3,
        out_shape=[jax.ShapeDtypeStruct(a.shape, a.dtype) for a in arrs],
        scratch_shapes=[pltpu.SemaphoreType.DMA((8,))],
        compiler_params=pltpu.CompilerParams(vmem_limit_bytes=4 * 2**20),
        name="copy_out",
    )(*arrs)


def solution(mesh):
    def local_block(hidden, tok_pos, norm_gain, w_query, w_key, w_value, w_out):
        results = attention_block(
            mesh, tok_pos.reshape(-1, HEAD), inv_freq_row(), norm_gain[None, :], hidden, w_key, w_value, w_query, w_out
        )
        return tuple(copy_out(*results))

    row_spec = P(("dp", "cp"), None)
    cache_spec = P(("dp", "cp"), "tp", None)
    return jax.shard_map(
        local_block,
        mesh=mesh,
        in_specs=(row_spec, P(("dp", "cp")), P(None), P(None, "tp"), P(None, "tp"), P(None, "tp"), P("tp", None)),
        out_specs=(row_spec, cache_spec, cache_spec),
        check_vma=False,
    )
```

```python
import functools

import jax
import jax.numpy as jnp
import numpy as np
from jax import lax
from jax.experimental import pallas as pl
from jax.experimental.pallas import tpu as pltpu
from jax.sharding import PartitionSpec as P

HEAD = 128
THETA = 1000000
EPS = 1e-5
NEG_BIG = -1e30
LOG2E = 1.4426950408889634
MESH = pl.DeviceIdType.MESH
VMEM_LIMIT = 64 * 2**20 - 64 * 2**10
POS_ROWS = 16
POS_BASE = 64
E_FRACTION = (3, 8)
N_Q = 4


def vmem_spec():
    return pl.BlockSpec(memory_space=pltpu.VMEM)


def any_spec():
    return pl.BlockSpec(memory_space=pl.ANY)


def inv_freq_row():
    freq = 1.0 / (np.float64(THETA) ** (np.arange(0, HEAD, 2) / HEAD))
    return jnp.asarray(np.concatenate([freq, freq])[None, :], jnp.float32)


def rope(head_f32, cos_full, sin_full):
    vals = head_f32.astype(jnp.bfloat16).astype(jnp.float32)
    return (vals * cos_full + pltpu.roll(vals, HEAD // 2, 1) * sin_full).astype(jnp.bfloat16)


def position_columns(pos_row):
    tiles = []
    for t in range(pos_row.shape[1] // HEAD):
        tile = jnp.broadcast_to(pos_row[:, t * HEAD : (t + 1) * HEAD], (HEAD, HEAD))
        tiles.append(jnp.transpose(tile))
    return jnp.concatenate(tiles, axis=0)


def block_kernel(
    n_tp, n_x, pos_hbm, freq_hbm, gain_hbm, hid_hbm, wk_hbm, wv_hbm, wq_hbm, wo_hbm, out, kc, vc,
    kv, r, cos, sin, wq, wr, we, ct, q, mx, ls, acc, acc_e, pos_q, pos_ref, freq_ref, gain_ref, ssem, rsem, lsem,
):
    rows, width = r.shape
    kv_cols = wk_hbm.shape[1]
    kv_heads = kv_cols // HEAD
    heads = wq_hbm.shape[1] // HEAD
    group = heads // kv_heads
    n_chunk, chunk = mx.shape[0], mx.shape[2] // group
    n_cp = 2 * n_x
    n_hop = 9
    n_ring = 26 + n_hop * n_tp
    half = rows // 2
    cols = wr.shape[2]
    e_cols = we.shape[3]
    piece = we.shape[2]
    q_cols = wq.shape[2]
    tp, cp = lax.axis_index("tp"), lax.axis_index("cp")
    x, core = cp // 2, cp % 2

    def at_x(dx, dc=0):
        return lax.rem(x + dx + n_x, n_x) * 2 + lax.rem(core + dc, 2)

    def at_y(dy):
        return lax.rem(tp + dy + n_tp, n_tp)

    x_right, x_left, partner = {"cp": at_x(1)}, {"cp": at_x(-1)}, {"cp": at_x(0, 1)}
    y_right, y_left, y_far = {"tp": at_y(1)}, {"tp": at_y(-1)}, {"tp": at_y(2)}

    def rc(src, dst, idx, dev, send=None):
        return pltpu.make_async_remote_copy(
            src_ref=src,
            dst_ref=dst,
            send_sem=ssem.at[idx if send is None else send],
            recv_sem=rsem.at[idx],
            device_id=dev,
            device_id_type=MESH,
        )

    def lc(src, dst, idx):
        return pltpu.make_async_copy(src, dst, lsem.at[idx])

    def part_of(i, size, sub=None):
        if sub is None:
            return pl.ds(pl.multiple_of(i * size, size), size)
        return pl.ds(pl.multiple_of(i * size + sub * (size // 2), size // 2), size // 2)

    quarter = half // 2
    parts = (slice(0, quarter), slice(quarter, half), slice(half, rows))
    r_cols = lambda t: pl.ds(pl.multiple_of(e_cols + t * cols, HEAD), cols)
    hid_copy = lambda i: lc(hid_hbm.at[parts[i]], out.at[parts[i]], i)
    wk_copy = lambda: lc(wk_hbm, wq.at[N_Q - 2], 3)
    wv_copy = lambda: lc(wv_hbm, wq.at[N_Q - 1], 4)
    wq_copy = lambda c: lc(wq_hbm.at[:, part_of(c, q_cols)], wq.at[c], 5 + c)
    wr_copy = lambda: lc(wo_hbm.at[:, r_cols(tp)], wr.at[0], 5 + N_Q)
    we_copy = lambda j: lc(wo_hbm.at[part_of(j, piece), pl.ds(0, e_cols)], we.at[j, 0], 6 + N_Q + j)

    top, low = pl.ds(0, half), pl.ds(half, half + POS_ROWS)
    top_a, top_b = pl.ds(0, quarter), pl.ds(quarter, quarter)
    k_cols, v_cols = pl.ds(0, kv_cols), pl.ds(kv_cols, kv_cols)
    low_a, low_b = pl.ds(half, quarter), pl.ds(half + quarter, quarter + POS_ROWS)

    def kv_copy(k):
        src, dst, dev = (
            ((0, top_a, v_cols), (2, top_a, v_cols), x_right),
            ((0, top_a, v_cols), (3, top_a, v_cols), x_left),
            ((0, low), (3, low), x_left),
            ((0, low), (2, low), x_right),
            ((0,), (1,), partner),
            ((2, top_a), (6, top_a), x_right),
            ((3, top_b), (6, top_b), x_left),
            ((2,), (4,), partner),
            ((3,), (5,), partner),
            ((6, top_a), (7, top_a), partner),
            ((0, top_b), (2, top_b), x_right),
            ((0, top_b), (3, top_b), x_left),
            ((2, low_a), (6, low_a), x_right),
            ((3, low_b), (6, low_b), x_left),
            ((6, top_b), (7, top_b), partner),
            ((6, low_a), (7, low_a), partner),
            ((6, low_b), (7, low_b), partner),
            ((0, top_a, k_cols), (2, top_a, k_cols), x_right),
            ((0, top_a, k_cols), (3, top_a, k_cols), x_left),
        )[k]
        return rc(kv.at[src], kv.at[dst], k if k < 10 else n_ring - 9 + k - 10, dev)

    y_devs = (y_right, y_left, y_far)
    mine = part_of(cp, piece)

    def wr_swap(k):
        return rc(wo_hbm.at[mine, r_cols(at_y((1, -1, 2)[k]))], wr.at[1 + k, mine], 10 + k, y_devs[k])

    def we_swap(k):
        if k < 2:
            return rc(wo_hbm.at[mine, pl.ds(0, e_cols)], we.at[cp, 1 + k], 13 + k, y_devs[k])
        sub = part_of(k - 2, piece // 2)
        return rc(we.at[cp, k - 1, sub], we.at[cp, 3, sub], 15 if k == 2 else 16 + n_hop * n_tp, y_devs[k - 2])

    own, right, left, far = cp, at_x(-1), at_x(1), at_x(2)
    ring = (
        (own, x_right, None), (own, x_left, None), (own, partner, None), (right, x_right, 0), (left, x_left, 1),
        (right, partner, None), (left, partner, None), (far, partner, 0), (far, partner, 1),
    )

    def wr_ring(m):
        src, dev, sub = ring[m]
        ref = wr.at[pl.ds(1, n_tp - 1), part_of(src, piece, sub)]
        return rc(ref, ref, 16 + m, dev)

    def we_ring(k, m):
        src, dev, sub = ring[m]
        ref = we.at[src, k] if sub is None else we.at[src, k, part_of(sub, piece // 2)]
        return rc(ref, ref, 16 + n_hop * k + m, dev)

    def start_own(copy):
        for m in range(3):
            copy(m).start()

    def pass_on(copy):
        copy(0).wait_recv()
        copy(3).start()
        copy(5).start()
        copy(1).wait_recv()
        copy(4).start()
        copy(6).start()

    def pass_far(copy):
        copy(3).wait_recv()
        copy(7).start()
        copy(4).wait_recv()
        copy(8).start()

    ctx_base = n_ring
    out_base = ctx_base + 4 * n_chunk

    def ctx_copy(i, k):
        src, dst, sub, dev = ((0, 1, None, y_right), (0, 2, None, y_left), (1, 3, 0, y_right), (2, 3, 1, y_left))[k]
        sl = part_of(i, chunk, sub)
        return rc(ct.at[src, sl], ct.at[dst, sl], ctx_base + 4 * i + k, dev, 4 * i + k)

    def res_copy(i, k):
        t, sub, dev = ((tp, None, y_right), (tp, None, y_left), (at_y(-1), 0, y_right), (at_y(1), 1, y_left))[k]
        ref = out.at[part_of(i, chunk, sub), r_cols(t)]
        return rc(ref, ref, out_base + 4 * i + k, dev, 4 * i + k)

    def forward(copy, i):
        copy(i, 0).wait_recv()
        copy(i, 2).start()
        copy(i, 1).wait_recv()
        copy(i, 3).start()

    def forward_res(i):
        ctx_copy(i, 2).wait_send()
        ctx_copy(i, 3).wait_send()
        forward(res_copy, i)

    barrier = pltpu.get_barrier_semaphore()
    peers = (x_right, x_left, partner) + y_devs
    for dev in peers:
        pl.semaphore_signal(barrier, inc=1, device_id=dev, device_id_type=MESH)
    small = [
        lc(a, b, 6 + N_Q + n_cp + t)
        for t, (a, b) in enumerate(((gain_hbm, gain_ref), (pos_hbm, pos_ref), (freq_hbm, freq_ref)))
    ]
    small[0].start()
    hid_copy(0).start()
    wv_copy().start()
    wk_copy().start()
    small[1].start()
    small[2].start()
    hid_copy(1).start()
    hid_copy(2).start()
    for c in range(N_Q - 2):
        wq_copy(c).start()

    def normalise(sl):
        hid = out[sl, :].astype(jnp.float32)
        scaled = hid * lax.rsqrt(jnp.mean(hid * hid, axis=-1, keepdims=True) + EPS)
        r[sl, :] = (scaled * gain_ref[...]).astype(jnp.bfloat16)

    def product(sl, w):
        return jnp.dot(r[sl, :], wq[w], preferred_element_type=jnp.float32)

    def put_v(sl, v):
        v = v.astype(jnp.bfloat16)
        kv[0, sl, kv_cols:] = v
        vc[sl] = jnp.stack([v[:, h * HEAD : (h + 1) * HEAD] for h in range(kv_heads)], axis=1)

    def put_k(sl, k):
        rots = []
        for h in range(kv_heads):
            rots.append(rope(k[:, h * HEAD : (h + 1) * HEAD], cos[sl, :], sin[sl, :]))
            kv[0, sl, h * HEAD : (h + 1) * HEAD] = rots[h]
        kc[sl] = jnp.stack(rots, axis=1)

    def project_kv(sl):
        k, v = product(sl, N_Q - 2), product(sl, N_Q - 1)
        put_v(sl, v)
        put_k(sl, k)

    small[0].wait()
    hid_copy(0).wait()
    normalise(parts[0])
    wv_copy().wait()
    put_v(parts[0], product(parts[0], N_Q - 1))
    pl.semaphore_wait(barrier, len(peers))
    kv_copy(0).start()
    kv_copy(1).start()
    for t in range(n_tp - 1):
        wr_swap(t).start()
    for t in range(2):
        we_swap(t).start()

    small[1].wait()
    small[2].wait()
    pos = pos_ref[...]
    pos_row = jnp.concatenate([pos[t : t + 1] for t in range(pos.shape[0])], axis=1)
    pos_q[...] = position_columns(pos_row.astype(jnp.float32))
    angles = pos_q[...] * freq_ref[...]
    lane = lax.broadcasted_iota(jnp.int32, angles.shape, 1)
    sines = jnp.sin(angles)
    cos[...] = jnp.cos(angles)
    sin[...] = jnp.where(lane < HEAD // 2, -sines, sines)
    hi = jnp.broadcast_to((pos_row // POS_BASE).astype(jnp.float32), (POS_ROWS // 2, rows))
    lo = jnp.broadcast_to(lax.rem(pos_row, POS_BASE).astype(jnp.float32), (POS_ROWS // 2, rows))
    kv[0, rows:, :] = jnp.concatenate([hi, lo], axis=0).astype(jnp.bfloat16)

    wk_copy().wait()
    put_k(parts[0], product(parts[0], N_Q - 2))
    kv_copy(17).start()
    kv_copy(18).start()
    hid_copy(1).wait()
    normalise(parts[1])
    project_kv(parts[1])
    kv_copy(10).start()
    kv_copy(11).start()
    hid_copy(2).wait()
    normalise(parts[2])
    project_kv(parts[2])
    kv_copy(2).start()
    kv_copy(3).start()
    kv_copy(4).start()
    for c in range(N_Q - 2, N_Q):
        wq_copy(c).start()
    wr_copy().start()
    for j in range(n_cp):
        we_copy(j).start()

    @pl.loop(0, N_Q)
    def _(c):
        wq_copy(c).wait()
        qc = jnp.dot(r[...], wq[c], preferred_element_type=jnp.float32)
        per = q_cols // HEAD
        for j in range(per):
            rot = rope(qc[:, j * HEAD : (j + 1) * HEAD], cos[...], sin[...])
            head = c * per + j
            kvh, g = head // group, lax.rem(head, group)
            for i in range(n_chunk):
                q[i, kvh, part_of(g, chunk), :] = rot[i * chunk : (i + 1) * chunk]

    mx[...] = jnp.full_like(mx, NEG_BIG)
    ls[...] = jnp.zeros_like(ls)
    acc[...] = jnp.zeros_like(acc)
    scale = HEAD**-0.5 * LOG2E

    def attend(i, slot, n_blk=1):
        pos_i = pos_q[part_of(i, chunk), :]
        n_l = n_blk * rows // HEAD
        biases = []
        for b in range(n_blk):
            hi = kv[slot + b, pl.ds(rows, POS_ROWS // 2), :].astype(jnp.float32)
            lo = kv[slot + b, pl.ds(rows + POS_ROWS // 2, POS_ROWS // 2), :].astype(jnp.float32)
            pos_k = (hi * POS_BASE + lo)[0:1, :]
            for t in range(rows // HEAD):
                biases.append(jnp.where(pos_k[:, t * HEAD : (t + 1) * HEAD] <= pos_i, 0.0, NEG_BIG))
        bias = jnp.concatenate(biases, axis=1)

        def block(b, first_col):
            return kv[slot + b, pl.ds(0, rows), first_col : first_col + HEAD]

        raw = [
            [
                lax.dot_general(
                    q[i, kvh], block(b, kvh * HEAD), (((1,), (1,)), ((), ())), preferred_element_type=jnp.float32
                )
                for b in range(n_blk)
            ]
            for kvh in range(kv_heads)
        ]
        for kvh in range(kv_heads):
            s = jnp.concatenate(raw[kvh], axis=1)
            s = (s.reshape(group, chunk, n_blk * rows) * scale + bias[None]).reshape(group * chunk, n_blk * rows)
            m_old = mx[i, kvh]
            m_new = jnp.maximum(m_old, jnp.max(s, axis=1, keepdims=True))
            alpha = jnp.exp2(m_old - m_new)
            p = jnp.exp2(s - jnp.concatenate([m_new] * n_l, axis=1))
            part = p[:, :HEAD]
            for t in range(1, n_l):
                part = part + p[:, t * HEAD : (t + 1) * HEAD]
            mx[i, kvh] = m_new
            ls[i, kvh] = ls[i, kvh] * alpha + part
            p = p.astype(jnp.bfloat16)
            pv = acc[i, kvh] * alpha
            for b in range(n_blk):
                pv = pv + jnp.dot(
                    p[:, b * rows : (b + 1) * rows], block(b, kv_cols + kvh * HEAD), preferred_element_type=jnp.float32
                )
            acc[i, kvh] = pv

    n_lead = n_chunk // 2

    def attend_each(chunks, slots):
        n_slot = slots[1] - slots[0]

        @pl.loop(0, (chunks[1] - chunks[0]) * n_slot)
        def _(t):
            attend(chunks[0] + t // n_slot, slots[0] + lax.rem(t, n_slot))

    def attend_some(i, first, last):
        @pl.loop(0, (last - first) // 2)
        def _(t):
            attend(i, first + 2 * t, 2)

    def finish(i):
        for kvh in range(kv_heads):
            total = jnp.sum(ls[i, kvh], axis=1, keepdims=True)
            ctx = (acc[i, kvh] / total).astype(jnp.bfloat16)
            for g in range(group):
                h = kvh * group + g
                ct[0, part_of(i, chunk), h * HEAD : (h + 1) * HEAD] = ctx[g * chunk : (g + 1) * chunk]
        ctx_copy(i, 0).start()
        ctx_copy(i, 1).start()

    kv_copy(0).wait_recv()
    kv_copy(17).wait_recv()
    kv_copy(5).start()
    attend_each((0, 1), (0, 1))
    kv_copy(11).wait_recv()
    kv_copy(6).start()
    kv_copy(10).wait_recv()
    kv_copy(1).wait_recv()
    kv_copy(18).wait_recv()
    attend_each((1, n_lead), (0, 1))
    kv_copy(4).wait_recv()
    attend_each((0, 1), (1, 2))
    kv_copy(3).wait_recv()
    kv_copy(12).start()
    kv_copy(7).start()
    kv_copy(2).wait_recv()
    kv_copy(13).start()
    kv_copy(8).start()
    attend_each((1, n_lead), (1, 2))
    attend_each((0, 1), (2, 4))
    kv_copy(5).wait_recv()
    kv_copy(9).start()
    kv_copy(6).wait_recv()
    kv_copy(14).start()
    kv_copy(7).wait_recv()
    kv_copy(8).wait_recv()
    for k in range(2):
        we_swap(k).wait_recv()
        we_swap(2 + k).start()
    attend_each((0, 1), (4, 5))
    for t in range(n_tp - 1):
        wr_swap(t).wait_recv()
    start_own(wr_ring)
    attend_each((0, 1), (5, 6))
    kv_copy(12).wait_recv()
    kv_copy(15).start()
    kv_copy(13).wait_recv()
    kv_copy(16).start()
    attend_each((0, 1), (6, 7))
    for k in (9, 14, 15, 16):
        kv_copy(k).wait_recv()
    attend_each((0, 1), (7, 8))
    for k in range(19):
        kv_copy(k).wait_send()
    for k in range(n_tp - 1):
        wr_swap(k).wait_send()
        we_swap(k).wait_send()
    finish(0)

    @pl.loop(1, n_lead)
    def _(i):
        attend_some(i, 2, n_cp)
        finish(i)

    we_k = lambda k: functools.partial(we_ring, k)
    for k in range(2, 4):
        we_swap(k).wait_recv()
    start_own(we_k(1))

    def late_chunk(i):
        attend_some(i, 0, n_cp // 2)
        forward(ctx_copy, i - n_lead)
        attend_some(i, n_cp // 2, n_cp)
        finish(i)

    late_chunk(n_lead)
    pass_on(wr_ring)
    for k in range(2, n_tp):
        start_own(we_k(k))
    late_chunk(n_lead + 1)
    pass_on(we_k(1))
    forward(ctx_copy, n_lead)
    pass_far(wr_ring)
    for m in (2, 5, 6, 7, 8):
        wr_ring(m).wait_recv()
    wr_copy().wait()

    def project_own(i):
        ctx_copy(i, 2).wait_recv()
        ctx_copy(i, 3).wait_recv()
        sl = part_of(i, chunk)
        proj = jnp.dot(ct[0, sl, :], wr[0], preferred_element_type=jnp.float32)
        for t in range(1, n_tp):
            proj = proj + jnp.dot(ct[t, sl, :], wr[t], preferred_element_type=jnp.float32)
        out[sl, r_cols(tp)] = (out[sl, r_cols(tp)].astype(jnp.float32) + proj).astype(jnp.bfloat16)
        for k in range(2):
            ctx_copy(i, k).wait_send()
            res_copy(i, k).start()

    project_loop = lambda lo, hi: pl.loop(lo, hi)(project_own)
    project_loop(0, n_chunk - 3)
    forward(ctx_copy, n_lead + 1)
    project_loop(n_chunk - 3, n_chunk - 2)
    pass_on(we_k(2))
    project_loop(n_chunk - 2, n_chunk)

    e_tile = 512
    n_e = e_cols // e_tile

    def project(j, first=False, last=False):
        ctx = jnp.concatenate([ct[t, :, part_of(j, piece)] for t in range(n_tp)], axis=1)

        @pl.loop(0, n_e)
        def _(n):
            sl = part_of(n, e_tile)
            w = we[j, :, :, sl].reshape(n_tp * piece, e_tile)
            add = jnp.dot(ctx, w, preferred_element_type=jnp.float32)
            if not first:
                add = acc_e[:, sl] + add
            if last:
                out[:, sl] = (out[:, sl].astype(jnp.float32) + add).astype(jnp.bfloat16)
            else:
                acc_e[:, sl] = add

    for j in range(n_cp):
        we_copy(j).wait()
    pass_on(we_k(3))
    project(own, first=True)
    forward_res(0)
    for k in range(1, n_tp):
        we_k(k)(2).wait_recv()
    project(at_x(0, 1))
    project(right)
    forward_res(1)
    pass_far(we_k(1))
    project(left)
    forward_res(2)
    pass_far(we_k(2))
    for k in range(1, n_tp):
        we_k(k)(5).wait_recv()
    project(at_x(-1, 1))
    for k in range(1, n_tp):
        we_k(k)(6).wait_recv()
    forward_res(3)
    project(at_x(1, 1))
    pass_far(we_k(3))
    project(far)
    for k in range(1, n_tp):
        we_k(k)(7).wait_recv()
        we_k(k)(8).wait_recv()
    project(at_x(2, 1), last=True)

    @pl.loop(0, n_chunk)
    def _(i):
        res_copy(i, 2).wait_recv()
        res_copy(i, 3).wait_recv()

    we_swap(3).wait_send()
    for m in range(n_hop):
        wr_ring(m).wait_send()
        for k in range(1, n_tp):
            we_ring(k, m).wait_send()

    @pl.loop(0, n_chunk)
    def _(i):
        for k in range(4):
            res_copy(i, k).wait_send()


def attention_block(mesh, pos, freq, gain, hidden, w_key, w_value, w_query, w_out):
    n_tp, n_cp = mesh.shape["tp"], mesh.shape["cp"]
    rows, width = hidden.shape
    kv_cols = w_key.shape[1]
    heads, kv_heads = w_query.shape[1] // HEAD, kv_cols // HEAD
    n_chunk = 4
    grp = heads // kv_heads * (rows // n_chunk)
    e_cols = width * E_FRACTION[0] // E_FRACTION[1]
    cols = (width - e_cols) // n_tp
    k_rows = w_out.shape[0]
    bf16, f32 = jnp.bfloat16, jnp.float32
    n_sem = 26 + 9 * n_tp + 8 * n_chunk
    cache = (rows, kv_heads, HEAD)
    return pl.pallas_call(
        functools.partial(block_kernel, n_tp, n_cp // 2),
        out_shape=[pltpu.VMEM(s, bf16) for s in ((rows, width), cache, cache)],
        in_specs=[any_spec()] * 8,
        out_specs=[vmem_spec()] * 3,
        scratch_shapes=[
            pltpu.VMEM((n_cp, rows + POS_ROWS, 2 * kv_cols), bf16),
            pltpu.VMEM((rows, width), bf16),
            pltpu.VMEM((rows, HEAD), f32),
            pltpu.VMEM((rows, HEAD), f32),
            pltpu.VMEM((N_Q, width, w_query.shape[1] // N_Q), bf16),
            pltpu.VMEM((n_tp, k_rows, cols), bf16),
            pltpu.VMEM((n_cp, n_tp, k_rows // n_cp, e_cols), bf16),
            pltpu.VMEM((n_tp, rows, k_rows), bf16),
            pltpu.VMEM((n_chunk, kv_heads, grp, HEAD), bf16),
            pltpu.VMEM((n_chunk, kv_heads, grp, HEAD), f32),
            pltpu.VMEM((n_chunk, kv_heads, grp, HEAD), f32),
            pltpu.VMEM((n_chunk, kv_heads, grp, HEAD), f32),
            pltpu.VMEM((rows, e_cols), f32),
            pltpu.VMEM((rows, HEAD), f32),
            pltpu.VMEM(pos.shape, pos.dtype),
            pltpu.VMEM(freq.shape, f32),
            pltpu.VMEM(gain.shape, f32),
            pltpu.SemaphoreType.DMA((n_sem - 8 * n_chunk,)),
            pltpu.SemaphoreType.DMA((n_sem,)),
            pltpu.SemaphoreType.DMA((9 + N_Q + n_cp,)),
        ],
        compiler_params=pltpu.CompilerParams(collective_id=0, has_side_effects=True, vmem_limit_bytes=VMEM_LIMIT - 5 * 2**20),
        name="attention_block",
    )(pos, freq, gain, hidden, w_key, w_value, w_query, w_out)


def copy_kernel(src, k_src, v_src, dst, k_dst, v_dst, sem):
    n = 4
    tile = src.shape[0] // n
    rows = lambda i: pl.ds(i * tile, tile)
    copies = [pltpu.make_async_copy(src.at[rows(i)], dst.at[rows(i)], sem.at[i]) for i in range(n)]
    copies.append(pltpu.make_async_copy(k_src, k_dst, sem.at[n]))
    copies.append(pltpu.make_async_copy(v_src, v_dst, sem.at[n + 1]))
    for cpy in copies:
        cpy.start()
    for cpy in copies:
        cpy.wait()


def copy_out(*arrs):
    arrs = [pltpu.with_memory_space_constraint(a, pltpu.VMEM) for a in arrs]
    return pl.pallas_call(
        copy_kernel,
        in_specs=[vmem_spec()] * 3,
        out_specs=[any_spec()] * 3,
        out_shape=[jax.ShapeDtypeStruct(a.shape, a.dtype) for a in arrs],
        scratch_shapes=[pltpu.SemaphoreType.DMA((8,))],
        compiler_params=pltpu.CompilerParams(vmem_limit_bytes=4 * 2**20),
        name="copy_out",
    )(*arrs)


def solution(mesh):
    def local_block(hidden, tok_pos, norm_gain, w_query, w_key, w_value, w_out):
        results = attention_block(
            mesh, tok_pos.reshape(-1, HEAD), inv_freq_row(), norm_gain[None, :], hidden, w_key, w_value, w_query, w_out
        )
        return tuple(copy_out(*results))

    row_spec = P(("dp", "cp"), None)
    cache_spec = P(("dp", "cp"), "tp", None)
    return jax.shard_map(
        local_block,
        mesh=mesh,
        in_specs=(row_spec, P(("dp", "cp")), P(None), P(None, "tp"), P(None, "tp"), P(None, "tp"), P("tp", None)),
        out_specs=(row_spec, cache_spec, cache_spec),
        check_vma=False,
    )
```
